256 devices in a mesh: expert: 16 (over x, y), dp: 16 (over z, core).
Axes of the slice: x: 4, y: 4, z: 8, core: 2. Of those that a mesh axis runs over, the one named last changes fastest.
Arguments:
- tokens: bfloat16 [2, 32768, 1280], P(None, ('expert', 'dp')), may hold values from -6 to 6
- modality: int32 [2, 32768], P(None, ('expert', 'dp')), may hold values from 0 to 1, as said below
- routes: int32 [2, 32768, 1], P(None, ('expert', 'dp')), may hold values from 0 to 15; in each aligned block of 128 rows (0 to 127, 128 to 255, ..., all dimensions but the last counted through in order) at most 16 rows name the same one
- router: bfloat16 [1280, 16], replicated, may hold values from -0.15625 to 0.15625
- w_in: bfloat16 [16, 1280, 5120], P('expert', 'dp'), may hold values from -0.15625 to 0.15625
- w_out: bfloat16 [16, 5120, 1280], P('expert', 'dp'), may hold values from -0.078125 to 0.078125
Outputs:
- mixed: bfloat16 [2, 32768, 1280], P(None, ('expert', 'dp'))
- load: float32 [2, 2, 16], replicated
The draws below stay inside these ranges and needn't reach their ends.
Inputs may be any that keep to these rules, and one draw needn't show every extreme that they name: `routes`: among the 128 tokens of one micro-batch on one device (aligned blocks of 128 rows), at most 16 are routed to any one expert. `modality`: in every aligned block of 128 tokens of a micro-batch, the number of text tokens lies between 32 and 96.
All inputs are finite; a program needn't handle non-finite values.
Results may differ from the reference program's by a relative error of at most 0.0057.
Values may be sent and summed in bfloat16 or wider, within the bound.
A program may use at most 192 MiB of HBM per device.

```python
import math
import jax
import jax.numpy as jnp
import numpy as np
from jax import lax

D = 1280
FF = 5120
MB = 2
TOK_MB = 128
EXPERTS = 16
CAP = 16
TOKENS = 32768


def draw_modality(key, part):
    n_blocks = TOKENS // TOK_MB
    scores = jax.random.randint(key, (MB, n_blocks, TOK_MB), 0, 1 << 20) * TOK_MB + jnp.arange(TOK_MB, dtype=jnp.int32)
    order = jnp.argsort(scores, axis=-1)
    ranked = jnp.argsort(order, axis=-1)
    texts = TOK_MB // 4 + TOK_MB // 2 * jnp.arange(n_blocks, dtype=jnp.int32) // max(n_blocks - 1, 1)
    return (ranked < texts[None, :, None]).astype(jnp.int32).reshape(MB, TOKENS)


def level_of(key, shape, cuts, least, largest):
    def one(axis_at, shards_of):
        heights = jax.random.uniform(jax.random.fold_in(jax.random.fold_in(key, 6), axis_at), (shards_of,), jnp.float32, least / len(cuts), largest / len(cuts))
        return jnp.repeat(jnp.exp(heights), shape[axis_at] // shards_of).reshape((-1,) + (1,) * (len(shape) - axis_at - 1))

    gain = one(*cuts[0])
    for cut in cuts[1:]:
        gain = gain * one(*cut)
    return gain


def shared_out(key, own, number, rows, count, top, reach, skew):
    order = jax.random.permutation(key, count)
    crowded, common = load_shares(count, rows * top, reach, skew, True), load_shares(count, rows * top, reach, skew, False)
    places = jnp.arange(count)

    def named(sizes, offset_by):
        used = int((sizes > 0).sum())
        fixed = max(1, used // 4)
        shifted = fixed + (places - fixed + offset_by * (used - fixed)) % max(1, count - fixed)
        return jnp.zeros((count,), jnp.int32).at[order[jnp.where(places < fixed, places, shifted)]].set(jnp.asarray(sizes, jnp.int32))

    sizes = jnp.where(number % 4 == 0, named(crowded, number // 4), named(common, number - number // 4 - 1))
    mixed = jax.random.permutation(jax.random.fold_in(own, 3), count)
    donor, sink = mixed[0:count // 2 * 2:2], mixed[1:count // 2 * 2:2]
    room = jnp.minimum(sizes[donor] - 1, reach - sizes[sink]) // 2
    room = jnp.where((donor == order[0]) | (sink == order[0]) | (sizes[sink] == 0), 0, jnp.maximum(room, 0))
    shifted = jax.random.randint(jax.random.fold_in(own, 4), (count // 2,), 0, 1 << 20) % (room + 1)
    sizes = sizes.at[donor].add(-shifted).at[sink].add(shifted)
    items = jnp.searchsorted(jnp.cumsum(sizes), jnp.arange(rows * top), side="right").astype(jnp.int32)
    listing = items.reshape(top, rows).T
    listing = listing[jax.random.permutation(jax.random.fold_in(own, 1), rows)]
    offset_by = jax.random.randint(jax.random.fold_in(own, 2), (rows, 1), 0, top)
    return jnp.take_along_axis(listing, (jnp.arange(top)[None, :] + offset_by) % top, axis=1)


def load_shares(number_of, total, most, skew, full):
    portions = [(1 << 20) // math.isqrt(grade ** skew) + 1 for grade in range(1, number_of + 1)]
    largest = most if full else min(most, max(-(-total // number_of), total * portions[0] // sum(portions)))
    least = 1 if total - largest >= number_of - 1 else 0
    given, rest = [largest] + [least] * (number_of - 1), total - largest - least * (number_of - 1)
    while rest > 0:
        candidates = [i for i in range(1, number_of) if given[i] < largest] or [i for i in range(1, number_of) if given[i] < most]
        pool, budget = sum([portions[i] for i in candidates]), rest
        for i in candidates:
            extra = min(most - given[i], max(1, budget * portions[i] // pool), rest)
            given[i] = given[i] + extra
            rest = rest - extra
    return np.array(given)


def gaussian(stream_key, shape, deviation, reach, pieces=(), kind=jnp.bfloat16):
    drawn = jax.random.normal(stream_key, shape, jnp.float32) * deviation
    if len(pieces) > 0:
        drawn = level_of(stream_key, shape, pieces, -0.22, 0.18) * drawn
    return jnp.clip(drawn, min=-reach, max=reach).astype(kind)


def setup_inputs(seed: int = 0) -> dict:
    streams_of = jax.random.split(jax.random.key(seed), 7)
    tokens = gaussian(streams_of[0], (MB, TOKENS, D), 1.0, 6.0, ((1, 256),))
    modality = draw_modality(jax.random.fold_in(streams_of[6], 71), 0)
    routes_keys = jax.random.split(jax.random.fold_in(streams_of[2], 1), MB * TOKENS // TOK_MB)
    routes_turns = jax.random.permutation(jax.random.fold_in(streams_of[2], 3), MB * TOKENS // TOK_MB)
    routes = jax.vmap(lambda own, number: shared_out(jax.random.fold_in(streams_of[2], 2), own, number, TOK_MB, EXPERTS, 1, CAP, 2))(routes_keys, routes_turns).reshape((MB, TOKENS, 1))
    router = gaussian(streams_of[3], (D, EXPERTS), D ** -0.5, 0.15625)
    w_in = gaussian(streams_of[4], (EXPERTS, D, FF), D ** -0.5, 0.15625, ((0, 16), (1, 16)))
    w_out = gaussian(streams_of[5], (EXPERTS, FF, D), FF ** -0.5, 0.078125, ((0, 16), (1, 16)))
    return dict(tokens=tokens, modality=modality, routes=routes, router=router, w_in=w_in, w_out=w_out)


def expert_mlp(operands):
    rows_in, weight_in, weight_out = operands
    pre_act = jnp.dot(rows_in, weight_in, preferred_element_type=jnp.float32)
    hidden = jax.nn.gelu(pre_act, approximate=True).astype(jnp.bfloat16)
    return jnp.dot(hidden, weight_out, preferred_element_type=jnp.float32).astype(jnp.bfloat16)


def reference(tokens, modality, routes, router, w_in, w_out):
    blocks = TOKENS // TOK_MB
    slot_bound = blocks * CAP
    mixed_list = []
    counts = jnp.zeros((2, EXPERTS), jnp.float32)
    prob_sums = jnp.zeros((2, EXPERTS), jnp.float32)
    modal_counts = jnp.zeros((2,), jnp.float32)
    for micro in range(MB):
        micro_tokens = tokens[micro]
        expert_ids = routes[micro, :, 0].astype(jnp.int32)
        logits = jnp.dot(micro_tokens, router, preferred_element_type=jnp.float32)
        onehot = (expert_ids[:, None] == jnp.arange(EXPERTS, dtype=jnp.int32)[None, :]).astype(jnp.float32)
        gating = jax.nn.sigmoid(jnp.sum(logits * onehot, axis=-1))
        running = jnp.cumsum(onehot.reshape(blocks, TOK_MB, EXPERTS), axis=1).reshape(TOKENS, EXPERTS)
        slot_pos = (jnp.sum(running * onehot, axis=-1) - 1.0).astype(jnp.int32)
        device = (jnp.arange(TOKENS, dtype=jnp.int32) // TOK_MB).astype(jnp.int32)
        position = (expert_ids * slot_bound + device * CAP + slot_pos).astype(jnp.int32)
        buffer = jnp.zeros((EXPERTS * slot_bound, D), jnp.bfloat16).at[position].set(micro_tokens)
        buffer = buffer.reshape(EXPERTS, slot_bound, D)
        result = lax.map(expert_mlp, (buffer, w_in, w_out)).reshape(EXPERTS * slot_bound, D)
        scaled = result[position].astype(jnp.float32) * gating[:, None]
        mixed_list.append(scaled.astype(jnp.bfloat16))
        exps = jnp.exp(logits)
        router_probs = exps / jnp.sum(exps, axis=-1, keepdims=True)
        modal_hot = (modality[micro][:, None] == jnp.arange(2, dtype=jnp.int32)[None, :]).astype(jnp.float32)
        counts = counts + jnp.dot(modal_hot.T, onehot, precision=lax.Precision.HIGHEST)
        prob_sums = prob_sums + jnp.dot(modal_hot.T, router_probs, precision=lax.Precision.HIGHEST)
        modal_counts = modal_counts + jnp.sum(modal_hot, axis=0)
    load = jnp.stack([EXPERTS * counts / modal_counts[:, None], EXPERTS * prob_sums / modal_counts[:, None]])
    return jnp.stack(mixed_list), load
```

```python
import functools
import math

import jax
import jax.numpy as jnp
from jax import lax
from jax.experimental import pallas as pl
from jax.experimental.pallas import tpu as pltpu
from jax.sharding import Mesh
from jax.sharding import PartitionSpec as P

NX, NY, NZ, NC = 4, 4, 8, 2
AXES = ("expert_0", "expert_1", "dp_0", "dp_1")
MESH = pl.DeviceIdType.MESH
CHUNKS_IN = 4
CHUNKS_OUT = 5
GELU_C = math.sqrt(2.0 / math.pi)


def gelu(v):
    return 0.5 * v * (1.0 + jnp.tanh(GELU_C * (v + 0.044715 * (v * v * v))))


def layer_kernel(
    tokens_ref, routes_ref, modality_ref, router_ref, w_in_ref, w_out_ref,
    mixed_ref, load_ref,
    win, wout, placer, gate, buffer, rows, hidden, served, returned,
    stat, stat_rx, stat_sum, stat_rx2,
    local_sem, ring_send, ring_recv, pair_send, pair_recv,
    disp_send, disp_recv, back_send, back_recv, stat_send, stat_recv,
):
    shard_in = w_in_ref.shape[1]
    shard_out = w_out_ref.shape[1]
    width = tokens_ref.shape[1]
    toks = tokens_ref.shape[0]
    experts = router_ref.shape[1]
    block = rows.shape[0] // experts
    cols_in = win.shape[2]
    cols_out = wout.shape[2]
    chunks = CHUNKS_IN + CHUNKS_OUT
    dps = NZ * NC

    ex, ey = lax.axis_index("expert_0"), lax.axis_index("expert_1")
    z, c = lax.axis_index("dp_0"), lax.axis_index("dp_1")
    me = ex * NY + ey
    mine = z * NC + c
    up, down = lax.rem(z + 1, NZ), lax.rem(z + NZ - 1, NZ)
    other = 1 - c

    def plane_peer(j):
        p = lax.rem(me + j, experts)
        return p, (p // NY, lax.rem(p, NY), z, c)

    def dp_peer(j):
        p = lax.rem(mine + j, dps)
        return p, (ex, ey, p // NC, lax.rem(p, NC))

    def piece(n, source_z, core, half=None):
        shard = source_z * NC + core
        if n < CHUNKS_IN:
            view = win.at[n, pl.ds(pl.multiple_of(shard * shard_in, 16), shard_in)]
            if half is not None:
                view = win.at[
                    n, pl.ds(pl.multiple_of(shard * shard_in, 16), shard_in),
                    pl.ds(half * (cols_in // 2), cols_in // 2)]
            return view
        if half is None:
            return wout.at[n - CHUNKS_IN, pl.ds(pl.multiple_of(shard * shard_out, 16), shard_out)]
        rows_half = shard_out // 2
        return wout.at[
            n - CHUNKS_IN,
            pl.ds(pl.multiple_of(shard * shard_out + half * rows_half, 16), rows_half)]

    def local_copy(n):
        if n < CHUNKS_IN:
            source = w_in_ref.at[0, :, pl.ds(n * cols_in, cols_in)]
        else:
            source = w_out_ref.at[0, :, pl.ds((n - CHUNKS_IN) * cols_out, cols_out)]
        return pltpu.make_async_copy(source, piece(n, z, c), local_sem.at[n])

    def source_of(direction, hop):
        return lax.rem(z + NZ - hop, NZ) if direction == 0 else lax.rem(z + hop, NZ)

    def ring_copy(n, direction, hop):
        half = direction if hop == NZ // 2 else None
        ref = piece(n, source_of(direction, hop - 1), c, half)
        return pltpu.make_async_remote_copy(
            src_ref=ref, dst_ref=ref,
            send_sem=ring_send.at[n, direction, hop - 1],
            recv_sem=ring_recv.at[n, direction, hop - 1],
            device_id=(ex, ey, up if direction == 0 else down, c), device_id_type=MESH)

    def ring_arrival(n, direction, hop):
        half = direction if hop == NZ // 2 else None
        ref = piece(n, source_of(direction, hop), c, half)
        return pltpu.make_async_remote_copy(
            src_ref=ref, dst_ref=ref,
            send_sem=ring_send.at[n, direction, hop - 1],
            recv_sem=ring_recv.at[n, direction, hop - 1],
            device_id=(ex, ey, up if direction == 0 else down, c), device_id_type=MESH)

    def pair_slots():
        slots = [(0, 0)]
        for hop in range(1, NZ // 2):
            slots += [(0, hop), (1, hop)]
        return slots + [(0, NZ // 2)]

    slot_of = {s: k for k, s in enumerate(pair_slots())}

    def pair_copy(n, direction, hop, core):
        ref = piece(n, source_of(direction, hop), core)
        k = slot_of[(direction, hop)]
        return pltpu.make_async_remote_copy(
            src_ref=ref, dst_ref=ref,
            send_sem=pair_send.at[n, k], recv_sem=pair_recv.at[n, k],
            device_id=(ex, ey, z, other), device_id_type=MESH)

    for n in range(chunks):
        local_copy(n).start()

    barrier = pltpu.get_barrier_semaphore()

    def greet_plane(j, carry):
        _, device = plane_peer(j)
        pl.semaphore_signal(barrier, inc=1, device_id=device, device_id_type=MESH)
        return carry

    def greet_dp(j, carry):
        _, device = dp_peer(j)
        pl.semaphore_signal(barrier, inc=1, device_id=device, device_id_type=MESH)
        return carry

    lax.fori_loop(1, dps, greet_dp, 0)
    lax.fori_loop(1, experts, greet_plane, 0)
    pl.semaphore_wait(barrier, experts + dps - 2)

    def send_own(n):
        local_copy(n).wait()
        for direction in range(2):
            ring_copy(n, direction, 1).start()
        pair_copy(n, 0, 0, c).start()

    send_own(0)

    tok = tokens_ref[...]
    logits = jnp.dot(tok, router_ref[...], preferred_element_type=jnp.float32)
    lane = lax.broadcasted_iota(jnp.int32, (toks, experts), 1)
    onehot = (routes_ref[...] == lane).astype(jnp.float32)
    chosen = jnp.sum(logits * onehot, axis=1, keepdims=True)
    gate[...] = jnp.broadcast_to(1.0 / (1.0 + jnp.exp(-chosen)), gate.shape)
    micro_rows = toks // 2
    row_i = lax.broadcasted_iota(jnp.int32, (toks, toks), 0)
    col_i = lax.broadcasted_iota(jnp.int32, (toks, toks), 1)
    first = jnp.where(row_i >= micro_rows, micro_rows, 0)
    earlier = ((col_i <= row_i) & (col_i >= first)).astype(jnp.bfloat16)
    running = jnp.dot(earlier, onehot.astype(jnp.bfloat16), preferred_element_type=jnp.float32)
    lane_f = lane.astype(jnp.float32)
    spot = jnp.sum((running - 1.0 + lane_f * block) * onehot, axis=1, keepdims=True)
    token_id = lax.broadcasted_iota(jnp.int32, (toks, 1), 0)
    spot = spot + jnp.where(token_id >= micro_rows, block // 2, 0).astype(jnp.float32)
    slots = lax.broadcasted_iota(jnp.int32, (toks, experts * block), 1).astype(jnp.float32)
    place = (spot == slots).astype(jnp.bfloat16)
    placer[...] = place
    buffer[...] = lax.dot_general(
        place, tok, (((0,), (0,)), ((), ())), preferred_element_type=jnp.float32
    ).astype(jnp.bfloat16)

    exps = jnp.exp(logits)
    probs = exps / jnp.sum(exps, axis=1, keepdims=True)
    stat[...] = jnp.zeros(stat.shape, jnp.float32)
    for k in range(2):
        modal = (modality_ref[...] == k).astype(jnp.float32)
        stat[k:k + 1, 0:experts] = jnp.sum(onehot * modal, axis=0, keepdims=True)
        stat[2 + k:3 + k, 0:experts] = jnp.sum(probs * modal, axis=0, keepdims=True)
        stat[4 + k:5 + k, 0:experts] = jnp.sum(
            jnp.broadcast_to(modal, (toks, experts)), axis=0, keepdims=True)

    def dispatch(j, carry):
        p, device = plane_peer(j)
        pltpu.make_async_remote_copy(
            src_ref=buffer.at[pl.ds(pl.multiple_of(p * block, 16), block)],
            dst_ref=rows.at[pl.ds(pl.multiple_of(me * block, 16), block)],
            send_sem=disp_send, recv_sem=disp_recv,
            device_id=device, device_id_type=MESH).start()
        return carry

    own_rows = pl.ds(pl.multiple_of(me * block, 16), block)
    rows[own_rows, :] = buffer[own_rows, :]
    lax.fori_loop(1, experts, dispatch, 0)

    def stat_plane(j, carry):
        _, device = plane_peer(j)
        pltpu.make_async_remote_copy(
            src_ref=stat, dst_ref=stat_rx.at[me], send_sem=stat_send.at[0],
            recv_sem=stat_recv.at[0], device_id=device, device_id_type=MESH).start()
        return carry

    def stat_dp(j, carry):
        _, device = dp_peer(j)
        pltpu.make_async_remote_copy(
            src_ref=stat_sum, dst_ref=stat_rx2.at[mine], send_sem=stat_send.at[1],
            recv_sem=stat_recv.at[1], device_id=device, device_id_type=MESH).start()
        return carry

    stat_rx[me] = stat[...]
    lax.fori_loop(1, experts, stat_plane, 0)

    def take(ref, sem):
        pltpu.make_async_copy(ref, ref, sem).wait()

    others = (experts - 1) * block

    def first_product(n):
        tile = 256

        def body(t, carry):
            at = pl.ds(pl.multiple_of(t * tile, tile), tile)
            acc = jnp.dot(rows[...], win[n, :, at], preferred_element_type=jnp.float32)
            to = pl.ds(pl.multiple_of(n * cols_in + t * tile, tile), tile)
            hidden[:, to] = gelu(acc).astype(jnp.bfloat16)
            return carry

        lax.fori_loop(0, cols_in // tile, body, 0)

    def send_back(n):
        def body(j, carry):
            p, device = plane_peer(j)
            pltpu.make_async_remote_copy(
                src_ref=served.at[n, pl.ds(pl.multiple_of(p * block, 16), block)],
                dst_ref=returned.at[n, pl.ds(pl.multiple_of(me * block, 16), block)],
                send_sem=back_send.at[n], recv_sem=back_recv.at[n],
                device_id=device, device_id_type=MESH).start()
            return carry

        lax.fori_loop(1, experts, body, 0)

    def combine(n):
        take(returned.at[n, pl.ds(0, others)], back_recv.at[n])
        combined = jnp.dot(placer[...], returned[n], preferred_element_type=jnp.float32)
        mixed_ref[:, n * cols_out:(n + 1) * cols_out] = (
            combined * gate[:, 0:1]).astype(jnp.bfloat16)

    def second_product(n):
        acc = jnp.dot(hidden[...], wout[n], preferred_element_type=jnp.float32)
        served[n] = acc.astype(jnp.bfloat16)
        returned[n, own_rows, :] = served[n, own_rows, :]
        if n > 0:
            combine(n - 1)
        send_back(n)

    last = NZ // 2
    for r in range(chunks + last):
        if 0 < r < chunks:
            send_own(r)
        for hop in range(1, last + 1):
            n = r - hop
            if not 0 <= n < chunks:
                continue
            for direction in range(2):
                ring_arrival(n, direction, hop).wait_recv()
                if hop < last - 1 or hop == last - 1:
                    ring_copy(n, direction, hop + 1).start()
                if hop < last:
                    pair_copy(n, direction, hop, c).start()
            if hop == last:
                pair_copy(n, 0, hop, c).start()
        if r == 1:
            take(rows.at[pl.ds(0, others)], disp_recv)
        if r == 2:
            take(stat_rx.at[pl.ds(0, experts - 1)], stat_recv.at[0])
            total = stat_rx[0]
            for p in range(1, experts):
                total = total + stat_rx[p]
            stat_sum[...] = total
            stat_rx2[mine] = total
        if r == 3:
            lax.fori_loop(1, dps, stat_dp, 0)
        if r == 5:
            take(stat_rx2.at[pl.ds(0, dps - 1)], stat_recv.at[1])
            total = stat_rx2[0]
            for p in range(1, dps):
                total = total + stat_rx2[p]
            modal_counts = total[4:6, 0:experts]
            load_ref[0:2, :] = experts * total[0:2, 0:experts] / modal_counts
            load_ref[2:4, :] = experts * total[2:4, 0:experts] / modal_counts
        n = r - last
        if n >= 0:
            for (direction, hop) in pair_slots():
                pair_copy(n, direction, hop, other).wait_recv()
            if n < CHUNKS_IN:
                first_product(n)
            else:
                second_product(n - CHUNKS_IN)

    for n in range(chunks):
        for direction in range(2):
            for hop in range(1, last + 1):
                ring_copy(n, direction, hop).wait_send()
        for (direction, hop) in pair_slots():
            pair_copy(n, direction, hop, c).wait_send()
    take(buffer.at[pl.ds(0, others)], disp_send)
    take(stat_rx.at[pl.ds(0, experts - 1)], stat_send.at[0])
    take(stat_rx2.at[pl.ds(0, dps - 1)], stat_send.at[1])
    for n in range(CHUNKS_OUT):
        take(served.at[n, pl.ds(0, others)], back_send.at[n])
    combine(CHUNKS_OUT - 1)


def on_device(tokens, modality, routes, router, w_in, w_out):
    micro_count, tok_count, model_width = tokens.shape
    experts = router.shape[1]
    capacity = 2 * tok_count // experts
    toks = micro_count * tok_count
    block = micro_count * capacity
    slots = experts * block
    ff = w_in.shape[2]
    cols_in, cols_out = ff // CHUNKS_IN, model_width // CHUNKS_OUT
    chunks = CHUNKS_IN + CHUNKS_OUT
    half = NZ // 2
    bf16, f32 = jnp.bfloat16, jnp.float32
    vmem = pl.BlockSpec(memory_space=pltpu.VMEM)
    hbm = pl.BlockSpec(memory_space=pltpu.HBM)
    dma = pltpu.SemaphoreType.DMA
    mixed, load = pl.pallas_call(
        layer_kernel,
        out_shape=(
            jax.ShapeDtypeStruct((toks, model_width), bf16),
            jax.ShapeDtypeStruct((4, experts), f32),
        ),
        in_specs=[vmem, vmem, vmem, vmem, hbm, hbm],
        out_specs=(vmem, vmem),
        scratch_shapes=[
            pltpu.VMEM((CHUNKS_IN, model_width, cols_in), bf16),
            pltpu.VMEM((CHUNKS_OUT, ff, cols_out), bf16),
            pltpu.VMEM((toks, slots), bf16),
            pltpu.VMEM((toks, 128), f32),
            pltpu.VMEM((slots, model_width), bf16),
            pltpu.VMEM((slots, model_width), bf16),
            pltpu.VMEM((slots, ff), bf16),
            pltpu.VMEM((CHUNKS_OUT, slots, cols_out), bf16),
            pltpu.VMEM((CHUNKS_OUT, slots, cols_out), bf16),
            pltpu.VMEM((8, 128), f32),
            pltpu.VMEM((experts, 8, 128), f32),
            pltpu.VMEM((8, 128), f32),
            pltpu.VMEM((NZ * NC, 8, 128), f32),
            dma((chunks,)),
            dma((chunks, 2, half)),
            dma((chunks, 2, half)),
            dma((chunks, NZ)),
            dma((chunks, NZ)),
            dma,
            dma,
            dma((CHUNKS_OUT,)),
            dma((CHUNKS_OUT,)),
            dma((2,)),
            dma((2,)),
        ],
        compiler_params=pltpu.CompilerParams(
            collective_id=0, has_side_effects=True, vmem_limit_bytes=60 * 1024 * 1024
        ),
        name="layer",
    )(
        tokens.reshape(toks, model_width),
        routes.reshape(toks, 1),
        modality.reshape(toks, 1),
        router,
        w_in,
        w_out,
    )
    return mixed.reshape(tokens.shape), load.reshape(2, 2, experts)


def solution(mesh):
    torus = Mesh(mesh.devices.reshape(NX, NY, NZ, NC), AXES)
    expert, dp, both = AXES[:2], AXES[2:], AXES
    in_specs = (
        P(None, both, None), P(None, both), P(None, both, None), P(),
        P(expert, dp, None), P(expert, dp, None),
    )
    out_specs = (P(None, both, None), P())
    return jax.shard_map(
        on_device, mesh=torus, in_specs=in_specs, out_specs=out_specs, check_vma=False
    )
```

```python
import functools
import math

import jax
import jax.numpy as jnp
from jax import lax
from jax.experimental import pallas as pl
from jax.experimental.pallas import tpu as pltpu
from jax.sharding import Mesh
from jax.sharding import PartitionSpec as P

NX, NY, NZ, NC = 4, 4, 8, 2
AXES = ("expert_0", "expert_1", "dp_0", "dp_1")
MESH = pl.DeviceIdType.MESH
CHUNKS_IN = 4
WIDTHS_OUT = (512, 384, 256, 128)
CHUNKS_OUT = len(WIDTHS_OUT)
VMEM_BYTES = 65900000
GELU_C = math.sqrt(2.0 / math.pi)


def gelu(v):
    return 0.5 * v * (1.0 + jnp.tanh(GELU_C * (v + 0.044715 * (v * v * v))))


def layer_kernel(
    tokens_ref, routes_ref, modality_ref, router_ref, w_in_ref, w_out_ref,
    mixed_ref, load_ref,
    win, wout, tok_buf, placer, gate, buffer, rows, hidden, partial, served, returned,
    stat, stat_rx, stat_sum, stat_rx2,
    tok_sem, local_sem, ring_send, ring_recv, pair_send, pair_recv,
    disp_send, disp_recv, back_send, back_recv, stat_send, stat_recv,
):
    shard_in = w_in_ref.shape[1]
    shard_out = w_out_ref.shape[1]
    width = tokens_ref.shape[1]
    toks = tokens_ref.shape[0]
    experts = router_ref.shape[0]
    block = rows.shape[0] // experts
    cols_in = win.shape[2]
    chunks = CHUNKS_IN + CHUNKS_OUT
    dps = NZ * NC

    ex, ey = lax.axis_index("expert_0"), lax.axis_index("expert_1")
    z, c = lax.axis_index("dp_0"), lax.axis_index("dp_1")
    me = ex * NY + ey
    mine = z * NC + c
    up, down = lax.rem(z + 1, NZ), lax.rem(z + NZ - 1, NZ)
    other = 1 - c

    def plane_peer(j):
        p = lax.rem(me + j, experts)
        return p, (p // NY, lax.rem(p, NY), z, c)

    def dp_peer(j):
        p = lax.rem(mine + j, dps)
        return p, (ex, ey, p // NC, lax.rem(p, NC))

    def piece(n, source_z, core, half=None):
        shard = source_z * NC + core
        if n < CHUNKS_IN:
            view = win.at[n, pl.ds(pl.multiple_of(shard * shard_in, 16), shard_in)]
            if half is not None:
                view = win.at[
                    n, pl.ds(pl.multiple_of(shard * shard_in, 16), shard_in),
                    pl.ds(half * (cols_in // 2), cols_in // 2)]
            return view
        if half is None:
            return wout[n - CHUNKS_IN].at[pl.ds(pl.multiple_of(shard * shard_out, 16), shard_out)]
        rows_half = shard_out // 2
        return wout[n - CHUNKS_IN].at[
            pl.ds(pl.multiple_of(shard * shard_out + half * rows_half, 16), rows_half)]

    def columns(n):
        return pl.ds(sum(WIDTHS_OUT[:n]), WIDTHS_OUT[n])

    def local_copy(n):
        if n < CHUNKS_IN:
            source = w_in_ref.at[0, :, pl.ds(n * cols_in, cols_in)]
        else:
            source = w_out_ref.at[0, :, columns(n - CHUNKS_IN)]
        return pltpu.make_async_copy(source, piece(n, z, c), local_sem.at[n])

    def source_of(direction, hop):
        return lax.rem(z + NZ - hop, NZ) if direction == 0 else lax.rem(z + hop, NZ)

    def ring_copy(n, direction, hop):
        half = direction if hop == NZ // 2 else None
        ref = piece(n, source_of(direction, hop - 1), c, half)
        return pltpu.make_async_remote_copy(
            src_ref=ref, dst_ref=ref,
            send_sem=ring_send.at[n, direction, hop - 1],
            recv_sem=ring_recv.at[n, direction, hop - 1],
            device_id=(ex, ey, up if direction == 0 else down, c), device_id_type=MESH)

    def ring_arrival(n, direction, hop):
        half = direction if hop == NZ // 2 else None
        ref = piece(n, source_of(direction, hop), c, half)
        return pltpu.make_async_remote_copy(
            src_ref=ref, dst_ref=ref,
            send_sem=ring_send.at[n, direction, hop - 1],
            recv_sem=ring_recv.at[n, direction, hop - 1],
            device_id=(ex, ey, up if direction == 0 else down, c), device_id_type=MESH)

    def pair_slots():
        slots = [(0, 0)]
        for hop in range(1, NZ // 2):
            slots += [(0, hop), (1, hop)]
        return slots + [(0, NZ // 2)]

    slot_of = {s: k for k, s in enumerate(pair_slots())}

    def pair_copy(n, direction, hop, core):
        ref = piece(n, source_of(direction, hop), core)
        k = slot_of[(direction, hop)]
        return pltpu.make_async_remote_copy(
            src_ref=ref, dst_ref=ref,
            send_sem=pair_send.at[n, k], recv_sem=pair_recv.at[n, k],
            device_id=(ex, ey, z, other), device_id_type=MESH)

    local_copy(0).start()
    tok_copy = pltpu.make_async_copy(tokens_ref, tok_buf, tok_sem)
    tok_copy.start()
    for n in range(1, chunks):
        local_copy(n).start()

    barrier = pltpu.get_barrier_semaphore()

    def greet_plane(j, carry):
        _, device = plane_peer(j)
        pl.semaphore_signal(barrier, inc=1, device_id=device, device_id_type=MESH)
        return carry

    def greet_dp(j, carry):
        _, device = dp_peer(j)
        pl.semaphore_signal(barrier, inc=1, device_id=device, device_id_type=MESH)
        return carry

    lax.fori_loop(1, dps, greet_dp, 0)
    lax.fori_loop(1, experts, greet_plane, 0)
    pl.semaphore_wait(barrier, experts + dps - 2)

    def send_own(n):
        local_copy(n).wait()
        for direction in range(2):
            ring_copy(n, direction, 1).start()
        pair_copy(n, 0, 0, c).start()

    send_own(0)
    send_own(1)

    tok_copy.wait()
    tok = tok_buf[...]
    logits = lax.dot_general(
        router_ref[...], tok, (((1,), (1,)), ((), ())), preferred_element_type=jnp.float32)
    micro = toks // 2
    route = jnp.concatenate([routes_ref[0], routes_ref[1]], axis=1)
    modality = jnp.concatenate([modality_ref[0:1, :], modality_ref[1:2, :]], axis=1)
    expert_id = lax.broadcasted_iota(jnp.int32, (experts, toks), 0)
    onehot = (route == expert_id).astype(jnp.float32)
    chosen = jnp.sum(logits * onehot, axis=0, keepdims=True)
    gating = 1.0 / (1.0 + jnp.exp(-chosen))
    for m in range(2):
        spread = jnp.broadcast_to(gating[:, m * micro:(m + 1) * micro], (micro, micro))
        gate[m * micro:(m + 1) * micro, :] = spread.T
    row_i = lax.broadcasted_iota(jnp.int32, (toks, toks), 0)
    col_i = lax.broadcasted_iota(jnp.int32, (toks, toks), 1)
    first = jnp.where(col_i >= micro, micro, 0)
    earlier = ((row_i <= col_i) & (row_i >= first)).astype(jnp.bfloat16)
    running = jnp.dot(onehot.astype(jnp.bfloat16), earlier, preferred_element_type=jnp.float32)
    spot = jnp.sum(
        (running - 1.0 + expert_id.astype(jnp.float32) * block) * onehot, axis=0, keepdims=True)
    token_id = lax.broadcasted_iota(jnp.int32, (1, toks), 1)
    spot = spot + jnp.where(token_id >= micro, block // 2, 0).astype(jnp.float32)
    slots = lax.broadcasted_iota(jnp.int32, (experts * block, toks), 0).astype(jnp.float32)
    place = (spot == slots).astype(jnp.bfloat16)
    placer[...] = place
    buffer[...] = jnp.dot(place, tok, preferred_element_type=jnp.float32).astype(jnp.bfloat16)

    exps = jnp.exp(logits)
    probs = exps / jnp.sum(exps, axis=0, keepdims=True)
    stat[...] = jnp.zeros(stat.shape, jnp.float32)
    for k in range(2):
        modal = (modality == k).astype(jnp.float32)
        stat[:, k:k + 1] = jnp.sum(onehot * modal, axis=1, keepdims=True)
        stat[:, 2 + k:3 + k] = jnp.sum(probs * modal, axis=1, keepdims=True)
        stat[:, 4 + k:5 + k] = jnp.sum(
            jnp.broadcast_to(modal, (experts, toks)), axis=1, keepdims=True)

    def dispatch(j, carry):
        p, device = plane_peer(j)
        pltpu.make_async_remote_copy(
            src_ref=buffer.at[pl.ds(pl.multiple_of(p * block, 16), block)],
            dst_ref=rows.at[pl.ds(pl.multiple_of(me * block, 16), block)],
            send_sem=disp_send, recv_sem=disp_recv,
            device_id=device, device_id_type=MESH).start()
        return carry

    own_rows = pl.ds(pl.multiple_of(me * block, 16), block)
    rows[own_rows, :] = buffer[own_rows, :]
    lax.fori_loop(1, experts, dispatch, 0)

    def stat_plane(j, carry):
        _, device = plane_peer(j)
        pltpu.make_async_remote_copy(
            src_ref=stat, dst_ref=stat_rx.at[me], send_sem=stat_send.at[0],
            recv_sem=stat_recv.at[0], device_id=device, device_id_type=MESH).start()
        return carry

    def stat_dp(j, carry):
        _, device = dp_peer(j)
        pltpu.make_async_remote_copy(
            src_ref=stat_sum, dst_ref=stat_rx2.at[mine], send_sem=stat_send.at[1],
            recv_sem=stat_recv.at[1], device_id=device, device_id_type=MESH).start()
        return carry

    stat_rx[me] = stat[...]
    lax.fori_loop(1, experts, stat_plane, 0)

    def take(ref, sem):
        pltpu.make_async_copy(ref, ref, sem).wait()

    others = (experts - 1) * block

    def first_product(n):
        tile = 256

        def body(t, carry):
            at = pl.ds(pl.multiple_of(t * tile, tile), tile)
            acc = jnp.dot(rows[...], win[n, :, at], preferred_element_type=jnp.float32)
            to = pl.ds(pl.multiple_of(n * cols_in + t * tile, tile), tile)
            hidden[:, to] = gelu(acc).astype(jnp.bfloat16)
            return carry

        lax.fori_loop(0, cols_in // tile, body, 0)

    def send_back(n):
        def body(j, carry):
            p, device = plane_peer(j)
            pltpu.make_async_remote_copy(
                src_ref=served[n].at[pl.ds(pl.multiple_of(p * block, 16), block)],
                dst_ref=returned[n].at[pl.ds(pl.multiple_of(me * block, 16), block)],
                send_sem=back_send.at[n], recv_sem=back_recv.at[n],
                device_id=device, device_id_type=MESH).start()
            return carry

        lax.fori_loop(1, experts, body, 0)

    def combine(n):
        take(returned[n].at[pl.ds(0, others)], back_recv.at[n])
        combined = lax.dot_general(
            placer[...], returned[n][...], (((0,), (0,)), ((), ())),
            preferred_element_type=jnp.float32)
        mixed_ref[:, columns(n)] = (combined * gate[:, 0:1]).astype(jnp.bfloat16)

    chip_out = NC * shard_out

    def term(n, source_z):
        at = pl.ds(pl.multiple_of(source_z * chip_out, 128), chip_out)
        return jnp.dot(hidden[:, at], wout[n][at, :], preferred_element_type=jnp.float32)

    def second_product_start(n):
        width = pl.ds(0, WIDTHS_OUT[n])
        partial[:, width] = term(n, z)

        def body(k, carry):
            partial[:, width] += term(n, lax.rem(z + NZ // 2 + k, NZ))
            return carry

        lax.fori_loop(1, NZ // 2, body, 0)
        lax.fori_loop(NZ // 2 + 1, NZ, body, 0)

    def second_product_end(n):
        acc = partial[:, pl.ds(0, WIDTHS_OUT[n])] + term(n, lax.rem(z + NZ // 2, NZ))
        served[n][...] = acc.astype(jnp.bfloat16)
        returned[n][own_rows, :] = served[n][own_rows, :]
        send_back(n)
        if n > 1:
            combine(n - 2)

    last = NZ // 2
    for r in range(1, chunks + last):
        if r < chunks - 1:
            send_own(r + 1)
        for hop in range(1, last):
            n = r - hop
            if not 0 <= n < chunks:
                continue
            for direction in range(2):
                ring_arrival(n, direction, hop).wait_recv()
                ring_copy(n, direction, hop + 1).start()
                pair_copy(n, direction, hop, c).start()
        if r == 2:
            take(stat_rx.at[pl.ds(0, experts - 1)], stat_recv.at[0])
            total = stat_rx[0]
            for p in range(1, experts):
                total = total + stat_rx[p]
            stat_sum[...] = total
            stat_rx2[mine] = total
        if r == 3:
            lax.fori_loop(1, dps, stat_dp, 0)
        if r == 5:
            take(stat_rx2.at[pl.ds(0, dps - 1)], stat_recv.at[1])
            total = stat_rx2[0]
            for p in range(1, dps):
                total = total + stat_rx2[p]
            flat = total.T
            modal_counts = flat[4:6, 0:experts]
            load_ref[0] = experts * flat[0:2, 0:experts] / modal_counts
            load_ref[1] = experts * flat[2:4, 0:experts] / modal_counts
        n = r - last
        if n < 0:
            continue
        slots_now = pair_slots()
        for (direction, hop) in slots_now[:-1]:
            pair_copy(n, direction, hop, other).wait_recv()
        if n >= CHUNKS_IN:
            second_product_start(n - CHUNKS_IN)
        for direction in range(2):
            ring_arrival(n, direction, last).wait_recv()
        pair_copy(n, 0, last, c).start()
        if n == 0:
            take(rows.at[pl.ds(0, others)], disp_recv)
        pair_copy(n, 0, last, other).wait_recv()
        if n < CHUNKS_IN:
            first_product(n)
        else:
            second_product_end(n - CHUNKS_IN)

    combine(CHUNKS_OUT - 2)
    combine(CHUNKS_OUT - 1)

    for n in range(chunks):
        for direction in range(2):
            for hop in range(1, last + 1):
                ring_copy(n, direction, hop).wait_send()
        for (direction, hop) in pair_slots():
            pair_copy(n, direction, hop, c).wait_send()
    take(buffer.at[pl.ds(0, others)], disp_send)
    take(stat_rx.at[pl.ds(0, experts - 1)], stat_send.at[0])
    take(stat_rx2.at[pl.ds(0, dps - 1)], stat_send.at[1])
    for n in range(CHUNKS_OUT):
        take(served[n].at[pl.ds(0, others)], back_send.at[n])


def on_device(tokens, modality, routes, router, w_in, w_out):
    micro_count, tok_count, model_width = tokens.shape
    experts = router.shape[1]
    capacity = 2 * tok_count // experts
    toks = micro_count * tok_count
    block = micro_count * capacity
    slots = experts * block
    ff = w_in.shape[2]
    cols_in = ff // CHUNKS_IN
    chunks = CHUNKS_IN + CHUNKS_OUT
    half = NZ // 2
    bf16, f32 = jnp.bfloat16, jnp.float32
    vmem = pl.BlockSpec(memory_space=pltpu.VMEM)
    hbm = pl.BlockSpec(memory_space=pltpu.HBM)
    dma = pltpu.SemaphoreType.DMA
    mixed, load = pl.pallas_call(
        layer_kernel,
        out_shape=(
            jax.ShapeDtypeStruct((toks, model_width), bf16),
            jax.ShapeDtypeStruct((2, 2, experts), f32),
        ),
        in_specs=[hbm, vmem, vmem, vmem, hbm, hbm],
        out_specs=(vmem, vmem),
        scratch_shapes=[
            pltpu.VMEM((CHUNKS_IN, model_width, cols_in), bf16),
            [pltpu.VMEM((ff, w), bf16) for w in WIDTHS_OUT],
            pltpu.VMEM((toks, model_width), bf16),
            pltpu.VMEM((slots, toks), bf16),
            pltpu.VMEM((toks, 128), f32),
            pltpu.VMEM((slots, model_width), bf16),
            pltpu.VMEM((slots, model_width), bf16),
            pltpu.VMEM((slots, ff), bf16),
            pltpu.VMEM((slots, max(WIDTHS_OUT)), f32),
            [pltpu.VMEM((slots, w), bf16) for w in WIDTHS_OUT],
            [pltpu.VMEM((slots, w), bf16) for w in WIDTHS_OUT],
            pltpu.VMEM((experts, 128), f32),
            pltpu.VMEM((experts, experts, 128), f32),
            pltpu.VMEM((experts, 128), f32),
            pltpu.VMEM((NZ * NC, experts, 128), f32),
            dma,
            dma((chunks,)),
            dma((chunks, 2, half)),
            dma((chunks, 2, half)),
            dma((chunks, NZ)),
            dma((chunks, NZ)),
            dma,
            dma,
            dma((CHUNKS_OUT,)),
            dma((CHUNKS_OUT,)),
            dma((2,)),
            dma((2,)),
        ],
        compiler_params=pltpu.CompilerParams(
            collective_id=0, has_side_effects=True, vmem_limit_bytes=VMEM_BYTES
        ),
        name="layer",
    )(
        tokens.reshape(toks, model_width),
        jnp.transpose(routes, (0, 2, 1)),
        modality,
        router.T,
        w_in,
        w_out,
    )
    return mixed.reshape(tokens.shape), load


def solution(mesh):
    torus = Mesh(mesh.devices.reshape(NX, NY, NZ, NC), AXES)
    expert, dp, both = AXES[:2], AXES[2:], AXES
    in_specs = (
        P(None, both, None), P(None, both), P(None, both, None), P(),
        P(expert, dp, None), P(expert, dp, None),
    )
    out_specs = (P(None, both, None), P())
    return jax.shard_map(
        on_device, mesh=torus, in_specs=in_specs, out_specs=out_specs, check_vma=False
    )
```

```python
import functools
import math

import jax
import jax.numpy as jnp
from jax import lax
from jax.experimental import pallas as pl
from jax.experimental.pallas import tpu as pltpu
from jax.sharding import Mesh
from jax.sharding import PartitionSpec as P

NX, NY, NZ, NC = 4, 4, 8, 2
AXES = ("expert_0", "expert_1", "dp_0", "dp_1")
MESH = pl.DeviceIdType.MESH
CHUNKS_IN = 4
WIDTHS_OUT = (512, 384, 256, 128)
CHUNKS_OUT = len(WIDTHS_OUT)
VMEM_BYTES = 65900000
GELU_C = math.sqrt(2.0 / math.pi)


def gelu(v):
    return 0.5 * v * (1.0 + jnp.tanh(GELU_C * (v + 0.044715 * (v * v * v))))


def layer_kernel(
    tokens_ref, routes_ref, modality_ref, router_ref, w_in_ref, w_out_ref,
    mixed_ref, load_ref,
    win, wout, tok_buf, placer, gate, buffer, rows, hidden, served, returned,
    stat, stat_rx, stat_sum, stat_rx2,
    tok_sem, local_sem, ring_send, ring_recv, pair_send, pair_recv,
    disp_send, disp_recv, back_send, back_recv, stat_send, stat_recv, row_in,
):
    shard_in = w_in_ref.shape[1]
    shard_out = w_out_ref.shape[1]
    width = tokens_ref.shape[1]
    toks = tokens_ref.shape[0]
    experts = router_ref.shape[0]
    block = rows.shape[0] // experts
    cols_in = win.shape[2]
    chunks = CHUNKS_IN + CHUNKS_OUT
    dps = NZ * NC

    ex, ey = lax.axis_index("expert_0"), lax.axis_index("expert_1")
    z, c = lax.axis_index("dp_0"), lax.axis_index("dp_1")
    me = ex * NY + ey
    mine = z * NC + c
    up, down = lax.rem(z + 1, NZ), lax.rem(z + NZ - 1, NZ)
    other = 1 - c

    def plane_peer(j):
        p = lax.rem(me + j, experts)
        return p, (p // NY, lax.rem(p, NY), z, c)

    def dp_peer(j):
        p = lax.rem(mine + j, dps)
        return p, (ex, ey, p // NC, lax.rem(p, NC))

    def piece(n, source_z, core, half=None):
        shard = source_z * NC + core
        if n < CHUNKS_IN:
            view = win.at[n, pl.ds(pl.multiple_of(shard * shard_in, 16), shard_in)]
            if half is not None:
                view = win.at[
                    n, pl.ds(pl.multiple_of(shard * shard_in, 16), shard_in),
                    pl.ds(half * (cols_in // 2), cols_in // 2)]
            return view
        if half is None:
            return wout[n - CHUNKS_IN].at[pl.ds(pl.multiple_of(shard * shard_out, 16), shard_out)]
        rows_half = shard_out // 2
        return wout[n - CHUNKS_IN].at[
            pl.ds(pl.multiple_of(shard * shard_out + half * rows_half, 16), rows_half)]

    def columns(n):
        return pl.ds(sum(WIDTHS_OUT[:n]), WIDTHS_OUT[n])

    def local_copy(n):
        if n < CHUNKS_IN:
            source = w_in_ref.at[0, :, pl.ds(n * cols_in, cols_in)]
        else:
            source = w_out_ref.at[0, :, columns(n - CHUNKS_IN)]
        return pltpu.make_async_copy(source, piece(n, z, c), local_sem.at[n])

    def source_of(direction, hop):
        return lax.rem(z + NZ - hop, NZ) if direction == 0 else lax.rem(z + hop, NZ)

    def ring_copy(n, direction, hop):
        half = direction if hop == NZ // 2 else None
        ref = piece(n, source_of(direction, hop - 1), c, half)
        return pltpu.make_async_remote_copy(
            src_ref=ref, dst_ref=ref,
            send_sem=ring_send.at[n, direction, hop - 1],
            recv_sem=ring_recv.at[n, direction, hop - 1],
            device_id=(ex, ey, up if direction == 0 else down, c), device_id_type=MESH)

    def ring_arrival(n, direction, hop):
        half = direction if hop == NZ // 2 else None
        ref = piece(n, source_of(direction, hop), c, half)
        return pltpu.make_async_remote_copy(
            src_ref=ref, dst_ref=ref,
            send_sem=ring_send.at[n, direction, hop - 1],
            recv_sem=ring_recv.at[n, direction, hop - 1],
            device_id=(ex, ey, up if direction == 0 else down, c), device_id_type=MESH)

    def pair_slots():
        slots = [(0, 0)]
        for hop in range(1, NZ // 2):
            slots += [(0, hop), (1, hop)]
        return slots + [(0, NZ // 2)]

    slot_of = {s: k for k, s in enumerate(pair_slots())}

    def pair_copy(n, direction, hop, core):
        ref = piece(n, source_of(direction, hop), core)
        k = slot_of[(direction, hop)]
        return pltpu.make_async_remote_copy(
            src_ref=ref, dst_ref=ref,
            send_sem=pair_send.at[n, k], recv_sem=pair_recv.at[n, k],
            device_id=(ex, ey, z, other), device_id_type=MESH)

    local_copy(0).start()
    tok_copy = pltpu.make_async_copy(tokens_ref, tok_buf, tok_sem)
    tok_copy.start()
    for n in range(1, chunks):
        local_copy(n).start()

    barrier = pltpu.get_barrier_semaphore()

    x_sides = [(lax.rem(ex + d, NX), ey, z, c) for d in (1, NX - 1)]
    y_sides = [(ex, lax.rem(ey + d, NY), z, c) for d in (1, NY - 1)]
    z_sides = [(ex, ey, up, c), (ex, ey, down, c), (ex, ey, z, other)]

    def signal_all(sem, devices):
        for device in devices:
            pl.semaphore_signal(sem, inc=1, device_id=device, device_id_type=MESH)

    signal_all(barrier, z_sides + x_sides + y_sides)
    pl.semaphore_wait(barrier, len(z_sides + x_sides + y_sides))

    def send_own(n):
        local_copy(n).wait()
        for direction in range(2):
            ring_copy(n, direction, 1).start()
        pair_copy(n, 0, 0, c).start()

    send_own(0)
    send_own(1)
    signal_all(row_in.at[0], x_sides)

    tok_copy.wait()
    tok = tok_buf[...]
    logits = lax.dot_general(
        router_ref[...], tok, (((1,), (1,)), ((), ())), preferred_element_type=jnp.float32)
    micro = toks // 2
    route = jnp.concatenate([routes_ref[0], routes_ref[1]], axis=1)
    modality = jnp.concatenate([modality_ref[0:1, :], modality_ref[1:2, :]], axis=1)
    expert_id = lax.broadcasted_iota(jnp.int32, (experts, toks), 0)
    onehot = (route == expert_id).astype(jnp.float32)
    chosen = jnp.sum(logits * onehot, axis=0, keepdims=True)
    gating = 1.0 / (1.0 + jnp.exp(-chosen))
    for m in range(2):
        spread = jnp.broadcast_to(gating[:, m * micro:(m + 1) * micro], (micro, micro))
        gate[m * micro:(m + 1) * micro, :] = spread.T
    row_i = lax.broadcasted_iota(jnp.int32, (toks, toks), 0)
    col_i = lax.broadcasted_iota(jnp.int32, (toks, toks), 1)
    first = jnp.where(col_i >= micro, micro, 0)
    earlier = ((row_i <= col_i) & (row_i >= first)).astype(jnp.bfloat16)
    running = jnp.dot(onehot.astype(jnp.bfloat16), earlier, preferred_element_type=jnp.float32)
    spot = jnp.sum(
        (running - 1.0 + expert_id.astype(jnp.float32) * block) * onehot, axis=0, keepdims=True)
    token_id = lax.broadcasted_iota(jnp.int32, (1, toks), 1)
    spot = spot + jnp.where(token_id >= micro, block // 2, 0).astype(jnp.float32)
    slots = lax.broadcasted_iota(jnp.int32, (experts * block, toks), 0).astype(jnp.float32)
    place = (spot == slots).astype(jnp.bfloat16)
    placer[...] = place.T
    buffer[...] = jnp.dot(place, tok, preferred_element_type=jnp.float32).astype(jnp.bfloat16)

    exps = jnp.exp(logits)
    probs = exps / jnp.sum(exps, axis=0, keepdims=True)
    stat[...] = jnp.zeros(stat.shape, jnp.float32)
    for k in range(2):
        modal = (modality == k).astype(jnp.float32)
        stat[:, k:k + 1] = jnp.sum(onehot * modal, axis=1, keepdims=True)
        stat[:, 2 + k:3 + k] = jnp.sum(probs * modal, axis=1, keepdims=True)
        stat[:, 4 + k:5 + k] = jnp.sum(
            jnp.broadcast_to(modal, (experts, toks)), axis=1, keepdims=True)

    pl.semaphore_wait(row_in.at[0], 2)
    signal_all(row_in.at[1], y_sides)
    pl.semaphore_wait(row_in.at[1], 2)
    signal_all(row_in.at[2], y_sides)

    def dispatch(j, carry):
        p, device = plane_peer(j)
        pltpu.make_async_remote_copy(
            src_ref=buffer.at[pl.ds(pl.multiple_of(p * block, 16), block)],
            dst_ref=rows.at[pl.ds(pl.multiple_of(me * block, 16), block)],
            send_sem=disp_send, recv_sem=disp_recv,
            device_id=device, device_id_type=MESH).start()
        return carry

    own_rows = pl.ds(pl.multiple_of(me * block, 16), block)
    rows[own_rows, :] = buffer[own_rows, :]
    pl.semaphore_wait(row_in.at[2], 2)
    lax.fori_loop(1, experts, dispatch, 0)

    def stat_plane(j, carry):
        _, device = plane_peer(j)
        pltpu.make_async_remote_copy(
            src_ref=stat, dst_ref=stat_rx.at[me], send_sem=stat_send.at[0],
            recv_sem=stat_recv.at[0], device_id=device, device_id_type=MESH).start()
        return carry

    def stat_dp(j, carry):
        _, device = dp_peer(j)
        pltpu.make_async_remote_copy(
            src_ref=stat_sum, dst_ref=stat_rx2.at[mine], send_sem=stat_send.at[1],
            recv_sem=stat_recv.at[1], device_id=device, device_id_type=MESH).start()
        return carry

    stat_rx[me] = stat[...]
    lax.fori_loop(1, experts, stat_plane, 0)

    def take(ref, sem):
        pltpu.make_async_copy(ref, ref, sem).wait()

    others = (experts - 1) * block

    def first_product(n):
        tile = 256

        def body(t, carry):
            at = pl.ds(pl.multiple_of(t * tile, tile), tile)
            acc = jnp.dot(rows[...], win[n, :, at], preferred_element_type=jnp.float32)
            to = pl.ds(pl.multiple_of(n * cols_in + t * tile, tile), tile)
            hidden[:, to] = gelu(acc).astype(jnp.bfloat16)
            return carry

        lax.fori_loop(0, cols_in // tile, body, 0)

    def apart(d):
        return min(d[0], NX - d[0]) + min(d[1], NY - d[1])

    steps = [(dx, dy) for dx in range(NX) for dy in range(NY) if (dx, dy) != (0, 0)]
    steps.sort(key=apart, reverse=True)

    def send_back(n):
        for dx, dy in steps:
            px, py = lax.rem(ex + dx, NX), lax.rem(ey + dy, NY)
            p, device = px * NY + py, (px, py, z, c)
            pltpu.make_async_remote_copy(
                src_ref=served[n].at[pl.ds(pl.multiple_of(p * block, 16), block)],
                dst_ref=returned[n].at[pl.ds(pl.multiple_of(me * block, 16), block)],
                send_sem=back_send.at[n], recv_sem=back_recv.at[n],
                device_id=device, device_id_type=MESH).start()

    def combine(n):
        take(returned[n].at[pl.ds(0, others)], back_recv.at[n])
        combined = jnp.dot(
            placer[...], returned[n][...], preferred_element_type=jnp.float32)
        mixed_ref[:, columns(n)] = (combined * gate[:, 0:1]).astype(jnp.bfloat16)

    def second_product(n):
        acc = jnp.dot(hidden[...], wout[n][...], preferred_element_type=jnp.float32)
        served[n][...] = acc.astype(jnp.bfloat16)
        returned[n][own_rows, :] = served[n][own_rows, :]
        send_back(n)
        if n > 1:
            combine(n - 2)

    def product(n):
        for (direction, hop) in pair_slots():
            pair_copy(n, direction, hop, other).wait_recv()
        if n < CHUNKS_IN:
            first_product(n)
        else:
            second_product(n - CHUNKS_IN)

    last = NZ // 2
    for r in range(1, chunks + last):
        if r < chunks - 1:
            send_own(r + 1)
        for hop in range(1, last):
            n = r - hop
            if not 0 <= n < chunks:
                continue
            for direction in range(2):
                ring_arrival(n, direction, hop).wait_recv()
                ring_copy(n, direction, hop + 1).start()
                pair_copy(n, direction, hop, c).start()
        n = r - last
        if n >= 0:
            for direction in range(2):
                ring_arrival(n, direction, last).wait_recv()
            pair_copy(n, 0, last, c).start()
        if n == 0:
            take(rows.at[pl.ds(0, others)], disp_recv)
            take(stat_rx.at[pl.ds(0, experts - 1)], stat_recv.at[0])
            total = stat_rx[0]
            for p in range(1, experts):
                total = total + stat_rx[p]
            stat_sum[...] = total
            stat_rx2[mine] = total
        if n >= 0:
            product(n)
        if n == 1:
            lax.fori_loop(1, dps, stat_dp, 0)
        if n == 3:
            take(stat_rx2.at[pl.ds(0, dps - 1)], stat_recv.at[1])
            total = stat_rx2[0]
            for p in range(1, dps):
                total = total + stat_rx2[p]
            flat = total.T
            modal_counts = flat[4:6, 0:experts]
            load_ref[0] = experts * flat[0:2, 0:experts] / modal_counts
            load_ref[1] = experts * flat[2:4, 0:experts] / modal_counts

    combine(CHUNKS_OUT - 2)
    combine(CHUNKS_OUT - 1)

    for n in range(chunks):
        for direction in range(2):
            for hop in range(1, last + 1):
                ring_copy(n, direction, hop).wait_send()
        for (direction, hop) in pair_slots():
            pair_copy(n, direction, hop, c).wait_send()
    take(buffer.at[pl.ds(0, others)], disp_send)
    take(stat_rx.at[pl.ds(0, experts - 1)], stat_send.at[0])
    take(stat_rx2.at[pl.ds(0, dps - 1)], stat_send.at[1])
    for n in range(CHUNKS_OUT):
        take(served[n].at[pl.ds(0, others)], back_send.at[n])


def on_device(tokens, modality, routes, router, w_in, w_out):
    micro_count, tok_count, model_width = tokens.shape
    experts = router.shape[1]
    capacity = 2 * tok_count // experts
    toks = micro_count * tok_count
    block = micro_count * capacity
    slots = experts * block
    ff = w_in.shape[2]
    cols_in = ff // CHUNKS_IN
    chunks = CHUNKS_IN + CHUNKS_OUT
    half = NZ // 2
    bf16, f32 = jnp.bfloat16, jnp.float32
    vmem = pl.BlockSpec(memory_space=pltpu.VMEM)
    hbm = pl.BlockSpec(memory_space=pltpu.HBM)
    dma = pltpu.SemaphoreType.DMA
    mixed, load = pl.pallas_call(
        layer_kernel,
        out_shape=(
            pltpu.VMEM((toks, model_width), bf16),
            pltpu.VMEM((2, 2, experts), f32),
        ),
        in_specs=[hbm, vmem, vmem, vmem, hbm, hbm],
        out_specs=(vmem, vmem),
        scratch_shapes=[
            pltpu.VMEM((CHUNKS_IN, model_width, cols_in), bf16),
            [pltpu.VMEM((ff, w), bf16) for w in WIDTHS_OUT],
            pltpu.VMEM((toks, model_width), bf16),
            pltpu.VMEM((toks, slots), bf16),
            pltpu.VMEM((toks, 128), f32),
            pltpu.VMEM((slots, model_width), bf16),
            pltpu.VMEM((slots, model_width), bf16),
            pltpu.VMEM((slots, ff), bf16),
            [pltpu.VMEM((slots, w), bf16) for w in WIDTHS_OUT],
            [pltpu.VMEM((slots, w), bf16) for w in WIDTHS_OUT],
            pltpu.VMEM((experts, 128), f32),
            pltpu.VMEM((experts, experts, 128), f32),
            pltpu.VMEM((experts, 128), f32),
            pltpu.VMEM((NZ * NC, experts, 128), f32),
            dma,
            dma((chunks,)),
            dma((chunks, 2, half)),
            dma((chunks, 2, half)),
            dma((chunks, NZ)),
            dma((chunks, NZ)),
            dma,
            dma,
            dma((CHUNKS_OUT,)),
            dma((CHUNKS_OUT,)),
            dma((2,)),
            dma((2,)),
            pltpu.SemaphoreType.REGULAR((3,)),
        ],
        compiler_params=pltpu.CompilerParams(
            collective_id=0, has_side_effects=True, vmem_limit_bytes=VMEM_BYTES
        ),
        name="layer",
    )(
        tokens.reshape(toks, model_width),
        jnp.transpose(routes, (0, 2, 1)),
        modality,
        router.T,
        w_in,
        w_out,
    )
    return mixed.reshape(tokens.shape), load


def solution(mesh):
    torus = Mesh(mesh.devices.reshape(NX, NY, NZ, NC), AXES)
    expert, dp, both = AXES[:2], AXES[2:], AXES
    in_specs = (
        P(None, both, None), P(None, both), P(None, both, None), P(),
        P(expert, dp, None), P(expert, dp, None),
    )
    out_specs = (P(None, both, None), P())
    return jax.shard_map(
        on_device, mesh=torus, in_specs=in_specs, out_specs=out_specs, check_vma=False
    )
```

```python
import functools
import math

import jax
import jax.numpy as jnp
from jax import lax
from jax.experimental import pallas as pl
from jax.experimental.pallas import tpu as pltpu
from jax.sharding import Mesh
from jax.sharding import PartitionSpec as P

NX, NY, NZ, NC = 4, 4, 8, 2
AXES = ("expert_0", "expert_1", "dp_0", "dp_1")
MESH = pl.DeviceIdType.MESH
CHUNKS_IN = 4
WIDTHS_OUT = (512, 384, 256, 128)
CHUNKS_OUT = len(WIDTHS_OUT)
VMEM_BYTES = 65900000
GELU_C = math.sqrt(2.0 / math.pi)


def gelu(v):
    return 0.5 * v * (1.0 + jnp.tanh(GELU_C * (v + 0.044715 * (v * v * v))))


def layer_kernel(
    tokens_ref, routes_hbm, modality_hbm, router_hbm, w_in_ref, w_out_ref,
    mixed_ref, load_ref,
    routes_ref, modality_ref, router_ref, win, wout, tok_buf, placer, gate, buffer, rows, hidden, served, returned,
    stat, stat_rx, stat_sum, stat_rx2,
    tok_sem, local_sem, ring_send, ring_recv, pair_send, pair_recv,
    disp_send, disp_recv, back_send, back_recv, stat_send, stat_recv, row_in, cross_send, cross_recv,
):
    shard_in = w_in_ref.shape[1]
    shard_out = w_out_ref.shape[1]
    width = tokens_ref.shape[1]
    toks = tokens_ref.shape[0]
    experts = router_hbm.shape[0]
    block = rows.shape[0] // experts
    cols_in = win.shape[2]
    chunks = CHUNKS_IN + CHUNKS_OUT
    dps = NZ * NC

    ex, ey = lax.axis_index("expert_0"), lax.axis_index("expert_1")
    z, c = lax.axis_index("dp_0"), lax.axis_index("dp_1")
    me = ex * NY + ey
    mine = z * NC + c
    up, down = lax.rem(z + 1, NZ), lax.rem(z + NZ - 1, NZ)
    other = 1 - c

    def plane_peer(j):
        p = lax.rem(me + j, experts)
        return p, (p // NY, lax.rem(p, NY), z, c)

    def dp_peer(j):
        p = lax.rem(mine + j, dps)
        return p, (ex, ey, p // NC, lax.rem(p, NC))

    def piece(n, source_z, core, half=None):
        shard = source_z * NC + core
        if n < CHUNKS_IN:
            view = win.at[n, pl.ds(pl.multiple_of(shard * shard_in, 16), shard_in)]
            if half is not None:
                view = win.at[
                    n, pl.ds(pl.multiple_of(shard * shard_in, 16), shard_in),
                    pl.ds(half * (cols_in // 2), cols_in // 2)]
            return view
        if half is None:
            return wout[n - CHUNKS_IN].at[pl.ds(pl.multiple_of(shard * shard_out, 16), shard_out)]
        rows_half = shard_out // 2
        return wout[n - CHUNKS_IN].at[
            pl.ds(pl.multiple_of(shard * shard_out + half * rows_half, 16), rows_half)]

    def columns(n):
        return pl.ds(sum(WIDTHS_OUT[:n]), WIDTHS_OUT[n])

    def local_copy(n):
        if n < CHUNKS_IN:
            source = w_in_ref.at[0, :, pl.ds(n * cols_in, cols_in)]
        else:
            source = w_out_ref.at[0, :, columns(n - CHUNKS_IN)]
        return pltpu.make_async_copy(source, piece(n, z, c), local_sem.at[n])

    def source_of(direction, hop):
        return lax.rem(z + NZ - hop, NZ) if direction == 0 else lax.rem(z + hop, NZ)

    def ring_copy(n, direction, hop):
        half = direction if hop == NZ // 2 else None
        ref = piece(n, source_of(direction, hop - 1), c, half)
        return pltpu.make_async_remote_copy(
            src_ref=ref, dst_ref=ref,
            send_sem=ring_send.at[n, direction, hop - 1],
            recv_sem=ring_recv.at[n, direction, hop - 1],
            device_id=(ex, ey, up if direction == 0 else down, c), device_id_type=MESH)

    def ring_arrival(n, direction, hop):
        half = direction if hop == NZ // 2 else None
        ref = piece(n, source_of(direction, hop), c, half)
        return pltpu.make_async_remote_copy(
            src_ref=ref, dst_ref=ref,
            send_sem=ring_send.at[n, direction, hop - 1],
            recv_sem=ring_recv.at[n, direction, hop - 1],
            device_id=(ex, ey, up if direction == 0 else down, c), device_id_type=MESH)

    def pair_slots():
        slots = [(0, 0)]
        for hop in range(1, NZ // 2):
            slots += [(0, hop), (1, hop)]
        return slots + [(0, NZ // 2)]

    slot_of = {s: k for k, s in enumerate(pair_slots())}

    def pair_copy(n, direction, hop, core):
        ref = piece(n, source_of(direction, hop), core)
        k = slot_of[(direction, hop)]
        return pltpu.make_async_remote_copy(
            src_ref=ref, dst_ref=ref,
            send_sem=pair_send.at[n, k], recv_sem=pair_recv.at[n, k],
            device_id=(ex, ey, z, other), device_id_type=MESH)

    barrier = pltpu.get_barrier_semaphore()

    x_sides = [(lax.rem(ex + d, NX), ey, z, c) for d in (1, NX - 1)]
    y_sides = [(ex, lax.rem(ey + d, NY), z, c) for d in (1, NY - 1)]
    z_sides = [(ex, ey, up, c), (ex, ey, down, c), (ex, ey, z, other)]

    def signal_all(sem, devices):
        for device in devices:
            pl.semaphore_signal(sem, inc=1, device_id=device, device_id_type=MESH)

    signal_all(barrier, z_sides + x_sides + y_sides)
    def cross_copy(n, direction, core, hop):
        ref = piece(n, source_of(direction, hop), core, direction)
        return pltpu.make_async_remote_copy(
            src_ref=ref, dst_ref=ref,
            send_sem=cross_send.at[direction], recv_sem=cross_recv.at[direction],
            device_id=(ex, ey, up if direction == 0 else down, other), device_id_type=MESH)

    local_copy(0).start()
    inputs = [(tokens_ref, tok_buf), (routes_hbm, routes_ref), (modality_hbm, modality_ref),
              (router_hbm, router_ref)]
    input_copies = [
        pltpu.make_async_copy(source, target, tok_sem.at[k])
        for k, (source, target) in enumerate(inputs)]
    for n in range(1, chunks):
        local_copy(n).start()
        if n == 1:
            for copy in input_copies:
                copy.start()
    pl.semaphore_wait(barrier, len(z_sides + x_sides + y_sides))

    def send_own(n):
        local_copy(n).wait()
        for direction in range(2):
            ring_copy(n, direction, 1).start()
        pair_copy(n, 0, 0, c).start()

    send_own(0)
    send_own(1)
    signal_all(row_in.at[0], x_sides)

    for copy in input_copies:
        copy.wait()
    tok = tok_buf[...]
    logits = lax.dot_general(
        router_ref[...], tok, (((1,), (1,)), ((), ())), preferred_element_type=jnp.float32)
    micro = toks // 2
    route = jnp.concatenate([routes_ref[0], routes_ref[1]], axis=1)
    modality = jnp.concatenate([modality_ref[0:1, :], modality_ref[1:2, :]], axis=1)
    expert_id = lax.broadcasted_iota(jnp.int32, (experts, toks), 0)
    onehot = (route == expert_id).astype(jnp.float32)
    chosen = jnp.sum(logits * onehot, axis=0, keepdims=True)
    gating = 1.0 / (1.0 + jnp.exp(-chosen))
    for m in range(2):
        spread = jnp.broadcast_to(gating[:, m * micro:(m + 1) * micro], (micro, micro))
        gate[m * micro:(m + 1) * micro, :] = spread.T
    row_i = lax.broadcasted_iota(jnp.int32, (toks, toks), 0)
    col_i = lax.broadcasted_iota(jnp.int32, (toks, toks), 1)
    first = jnp.where(col_i >= micro, micro, 0)
    earlier = ((row_i <= col_i) & (row_i >= first)).astype(jnp.bfloat16)
    running = jnp.dot(onehot.astype(jnp.bfloat16), earlier, preferred_element_type=jnp.float32)
    spot = jnp.sum(
        (running - 1.0 + expert_id.astype(jnp.float32) * block) * onehot, axis=0, keepdims=True)
    token_id = lax.broadcasted_iota(jnp.int32, (1, toks), 1)
    spot = spot + jnp.where(token_id >= micro, block // 2, 0).astype(jnp.float32)
    slots = lax.broadcasted_iota(jnp.int32, (experts * block, toks), 0).astype(jnp.float32)
    place = (spot == slots).astype(jnp.bfloat16)
    placer[...] = place.T
    buffer[...] = jnp.dot(place, tok, preferred_element_type=jnp.float32).astype(jnp.bfloat16)

    exps = jnp.exp(logits)
    probs = exps / jnp.sum(exps, axis=0, keepdims=True)
    stat[...] = jnp.zeros(stat.shape, jnp.float32)
    for k in range(2):
        modal = (modality == k).astype(jnp.float32)
        stat[:, k:k + 1] = jnp.sum(onehot * modal, axis=1, keepdims=True)
        stat[:, 2 + k:3 + k] = jnp.sum(probs * modal, axis=1, keepdims=True)
        stat[:, 4 + k:5 + k] = jnp.sum(
            jnp.broadcast_to(modal, (experts, toks)), axis=1, keepdims=True)

    pl.semaphore_wait(row_in.at[0], 2)
    signal_all(row_in.at[1], y_sides)
    pl.semaphore_wait(row_in.at[1], 2)
    signal_all(row_in.at[2], y_sides)

    def dispatch(j, carry):
        p, device = plane_peer(j)
        pltpu.make_async_remote_copy(
            src_ref=buffer.at[pl.ds(pl.multiple_of(p * block, 16), block)],
            dst_ref=rows.at[pl.ds(pl.multiple_of(me * block, 16), block)],
            send_sem=disp_send, recv_sem=disp_recv,
            device_id=device, device_id_type=MESH).start()
        return carry

    own_rows = pl.ds(pl.multiple_of(me * block, 16), block)
    rows[own_rows, :] = buffer[own_rows, :]
    pl.semaphore_wait(row_in.at[2], 2)
    lax.fori_loop(1, experts, dispatch, 0)

    def stat_plane(j, carry):
        _, device = plane_peer(j)
        pltpu.make_async_remote_copy(
            src_ref=stat, dst_ref=stat_rx.at[me], send_sem=stat_send.at[0],
            recv_sem=stat_recv.at[0], device_id=device, device_id_type=MESH).start()
        return carry

    def stat_dp(j, carry):
        _, device = dp_peer(j)
        pltpu.make_async_remote_copy(
            src_ref=stat_sum, dst_ref=stat_rx2.at[mine], send_sem=stat_send.at[1],
            recv_sem=stat_recv.at[1], device_id=device, device_id_type=MESH).start()
        return carry

    stat_rx[me] = stat[...]
    lax.fori_loop(1, experts, stat_plane, 0)

    def take(ref, sem):
        pltpu.make_async_copy(ref, ref, sem).wait()

    others = (experts - 1) * block

    def first_product(n):
        tile = 256

        def body(t, carry):
            at = pl.ds(pl.multiple_of(t * tile, tile), tile)
            acc = jnp.dot(rows[...], win[n, :, at], preferred_element_type=jnp.float32)
            to = pl.ds(pl.multiple_of(n * cols_in + t * tile, tile), tile)
            hidden[:, to] = gelu(acc).astype(jnp.bfloat16)
            return carry

        lax.fori_loop(0, cols_in // tile, body, 0)

    def apart(d):
        return min(d[0], NX - d[0]) + min(d[1], NY - d[1])

    steps = [(dx, dy) for dx in range(NX) for dy in range(NY) if (dx, dy) != (0, 0)]
    steps.sort(key=apart, reverse=True)

    def send_back(n):
        for dx, dy in steps:
            px, py = lax.rem(ex + dx, NX), lax.rem(ey + dy, NY)
            p, device = px * NY + py, (px, py, z, c)
            pltpu.make_async_remote_copy(
                src_ref=served[n].at[pl.ds(pl.multiple_of(p * block, 16), block)],
                dst_ref=returned[n].at[pl.ds(pl.multiple_of(me * block, 16), block)],
                send_sem=back_send.at[n], recv_sem=back_recv.at[n],
                device_id=device, device_id_type=MESH).start()

    def combine(n):
        take(returned[n].at[pl.ds(0, others)], back_recv.at[n])
        combined = jnp.dot(
            placer[...], returned[n][...], preferred_element_type=jnp.float32)
        mixed_ref[:, columns(n)] = (combined * gate[:, 0:1]).astype(jnp.bfloat16)

    def second_product(n):
        acc = jnp.dot(hidden[...], wout[n][...], preferred_element_type=jnp.float32)
        served[n][...] = acc.astype(jnp.bfloat16)
        returned[n][own_rows, :] = served[n][own_rows, :]
        send_back(n)
        if n > 1:
            combine(n - 2)

    def product(n):
        for (direction, hop) in pair_slots():
            if n < chunks - 1 or hop < last:
                pair_copy(n, direction, hop, other).wait_recv()
        if n == chunks - 1:
            for direction in range(2):
                cross_copy(n, direction, other, last).wait_recv()
        if n < CHUNKS_IN:
            first_product(n)
        else:
            second_product(n - CHUNKS_IN)

    last = NZ // 2
    for r in range(1, chunks + last):
        if r < chunks - 1:
            send_own(r + 1)
        for hop in range(1, last):
            n = r - hop
            if not 0 <= n < chunks:
                continue
            for direction in range(2):
                ring_arrival(n, direction, hop).wait_recv()
                ring_copy(n, direction, hop + 1).start()
                if n == chunks - 1 and hop == last - 1:
                    cross_copy(n, direction, c, hop).start()
                pair_copy(n, direction, hop, c).start()
        n = r - last
        if n >= 0:
            for direction in range(2):
                ring_arrival(n, direction, last).wait_recv()
            if n < chunks - 1:
                pair_copy(n, 0, last, c).start()
        if n == 0:
            take(rows.at[pl.ds(0, others)], disp_recv)
            take(stat_rx.at[pl.ds(0, experts - 1)], stat_recv.at[0])
            total = stat_rx[0]
            for p in range(1, experts):
                total = total + stat_rx[p]
            stat_sum[...] = total
            stat_rx2[mine] = total
        if n >= 0:
            product(n)
        if n == 1:
            lax.fori_loop(1, dps, stat_dp, 0)
        if n == 3:
            take(stat_rx2.at[pl.ds(0, dps - 1)], stat_recv.at[1])
            total = stat_rx2[0]
            for p in range(1, dps):
                total = total + stat_rx2[p]
            flat = total.T
            modal_counts = flat[4:6, 0:experts]
            load_ref[0] = experts * flat[0:2, 0:experts] / modal_counts
            load_ref[1] = experts * flat[2:4, 0:experts] / modal_counts

    for n in range(chunks):
        for direction in range(2):
            for hop in range(1, last + 1):
                ring_copy(n, direction, hop).wait_send()
        for (direction, hop) in pair_slots():
            if n < chunks - 1 or hop < last:
                pair_copy(n, direction, hop, c).wait_send()
    for direction in range(2):
        cross_copy(chunks - 1, direction, c, last - 1).wait_send()
    take(buffer.at[pl.ds(0, others)], disp_send)
    take(stat_rx.at[pl.ds(0, experts - 1)], stat_send.at[0])
    take(stat_rx2.at[pl.ds(0, dps - 1)], stat_send.at[1])
    combine(CHUNKS_OUT - 2)
    combine(CHUNKS_OUT - 1)
    for n in range(CHUNKS_OUT):
        take(served[n].at[pl.ds(0, others)], back_send.at[n])


def on_device(tokens, modality, routes, router, w_in, w_out):
    micro_count, tok_count, model_width = tokens.shape
    experts = router.shape[1]
    capacity = 2 * tok_count // experts
    toks = micro_count * tok_count
    block = micro_count * capacity
    slots = experts * block
    ff = w_in.shape[2]
    cols_in = ff // CHUNKS_IN
    chunks = CHUNKS_IN + CHUNKS_OUT
    half = NZ // 2
    bf16, f32 = jnp.bfloat16, jnp.float32
    vmem = pl.BlockSpec(memory_space=pltpu.VMEM)
    hbm = pl.BlockSpec(memory_space=pltpu.HBM)
    dma = pltpu.SemaphoreType.DMA
    mixed, load = pl.pallas_call(
        layer_kernel,
        out_shape=(
            pltpu.VMEM((toks, model_width), bf16),
            pltpu.VMEM((2, 2, experts), f32),
        ),
        in_specs=[hbm] * 6,
        out_specs=(vmem, vmem),
        scratch_shapes=[
            pltpu.VMEM((micro_count, 1, tok_count), jnp.int32),
            pltpu.VMEM((micro_count, tok_count), jnp.int32),
            pltpu.VMEM((experts, model_width), bf16),
            pltpu.VMEM((CHUNKS_IN, model_width, cols_in), bf16),
            [pltpu.VMEM((ff, w), bf16) for w in WIDTHS_OUT],
            pltpu.VMEM((toks, model_width), bf16),
            pltpu.VMEM((toks, slots), bf16),
            pltpu.VMEM((toks, 128), f32),
            pltpu.VMEM((slots, model_width), bf16),
            pltpu.VMEM((slots, model_width), bf16),
            pltpu.VMEM((slots, ff), bf16),
            [pltpu.VMEM((slots, w), bf16) for w in WIDTHS_OUT],
            [pltpu.VMEM((slots, w), bf16) for w in WIDTHS_OUT],
            pltpu.VMEM((experts, 128), f32),
            pltpu.VMEM((experts, experts, 128), f32),
            pltpu.VMEM((experts, 128), f32),
            pltpu.VMEM((NZ * NC, experts, 128), f32),
            dma((4,)),
            dma((chunks,)),
            dma((chunks, 2, half)),
            dma((chunks, 2, half)),
            dma((chunks, NZ)),
            dma((chunks, NZ)),
            dma,
            dma,
            dma((CHUNKS_OUT,)),
            dma((CHUNKS_OUT,)),
            dma((2,)),
            dma((2,)),
            pltpu.SemaphoreType.REGULAR((3,)),
            dma((2,)),
            dma((2,)),
        ],
        compiler_params=pltpu.CompilerParams(
            collective_id=0, has_side_effects=True, vmem_limit_bytes=VMEM_BYTES
        ),
        name="layer",
    )(
        tokens.reshape(toks, model_width),
        jnp.transpose(routes, (0, 2, 1)),
        modality,
        router.T,
        w_in,
        w_out,
    )
    return mixed.reshape(tokens.shape), load


def solution(mesh):
    torus = Mesh(mesh.devices.reshape(NX, NY, NZ, NC), AXES)
    expert, dp, both = AXES[:2], AXES[2:], AXES
    in_specs = (
        P(None, both, None), P(None, both), P(None, both, None), P(),
        P(expert, dp, None), P(expert, dp, None),
    )
    out_specs = (P(None, both, None), P())
    return jax.shard_map(
        on_device, mesh=torus, in_specs=in_specs, out_specs=out_specs, check_vma=False
    )
```

```python
import functools
import math

import jax
import jax.numpy as jnp
from jax import lax
from jax.experimental import pallas as pl
from jax.experimental.pallas import tpu as pltpu
from jax.sharding import Mesh
from jax.sharding import PartitionSpec as P

NX, NY, NZ, NC = 4, 4, 8, 2
AXES = ("expert_0", "expert_1", "dp_0", "dp_1")
MESH = pl.DeviceIdType.MESH
CHUNKS_IN = 2
WIDTHS_OUT = (512, 384, 256, 128)
CHUNKS_OUT = len(WIDTHS_OUT)
VMEM_BYTES = 65900000
GELU_C = math.sqrt(2.0 / math.pi)


def gelu(v):
    return 0.5 * v * (1.0 + jnp.tanh(GELU_C * (v + 0.044715 * (v * v * v))))


def layer_kernel(
    tokens_ref, routes_hbm, modality_hbm, router_hbm, w_in_ref, w_out_ref,
    mixed_ref, load_ref,
    routes_ref, modality_ref, router_ref, win, wout, tok_buf, placer, gate, buffer, rows, hidden, partial, served, returned,
    stat, stat_rx, stat_sum, stat_rx2,
    tok_sem, local_sem, ring_send, ring_recv, pair_send, pair_recv,
    disp_send, disp_recv, back_send, back_recv, stat_send, stat_recv, row_in, cross_send, cross_recv,
):
    shard_in = w_in_ref.shape[1]
    shard_out = w_out_ref.shape[1]
    width = tokens_ref.shape[1]
    toks = tokens_ref.shape[0]
    experts = router_hbm.shape[0]
    block = rows.shape[0] // experts
    cols_in = win.shape[2]
    chunks = CHUNKS_IN + CHUNKS_OUT
    dps = NZ * NC

    ex, ey = lax.axis_index("expert_0"), lax.axis_index("expert_1")
    z, c = lax.axis_index("dp_0"), lax.axis_index("dp_1")
    me = ex * NY + ey
    mine = z * NC + c
    up, down = lax.rem(z + 1, NZ), lax.rem(z + NZ - 1, NZ)
    other = 1 - c

    def plane_peer(j):
        p = lax.rem(me + j, experts)
        return p, (p // NY, lax.rem(p, NY), z, c)

    def dp_peer(j):
        p = lax.rem(mine + j, dps)
        return p, (ex, ey, p // NC, lax.rem(p, NC))

    def piece(n, source_z, core, half=None):
        shard = source_z * NC + core
        if n < CHUNKS_IN:
            view = win.at[n, pl.ds(pl.multiple_of(shard * shard_in, 16), shard_in)]
            if half is not None:
                view = win.at[
                    n, pl.ds(pl.multiple_of(shard * shard_in, 16), shard_in),
                    pl.ds(half * (cols_in // 2), cols_in // 2)]
            return view
        if half is None:
            return wout[n - CHUNKS_IN].at[pl.ds(pl.multiple_of(shard * shard_out, 16), shard_out)]
        rows_half = shard_out // 2
        return wout[n - CHUNKS_IN].at[
            pl.ds(pl.multiple_of(shard * shard_out + half * rows_half, 16), rows_half)]

    def columns(n):
        return pl.ds(sum(WIDTHS_OUT[:n]), WIDTHS_OUT[n])

    def local_copy(n):
        if n < CHUNKS_IN:
            source = w_in_ref.at[0, :, pl.ds(n * cols_in, cols_in)]
        else:
            source = w_out_ref.at[0, :, columns(n - CHUNKS_IN)]
        return pltpu.make_async_copy(source, piece(n, z, c), local_sem.at[n])

    def source_of(direction, hop):
        return lax.rem(z + NZ - hop, NZ) if direction == 0 else lax.rem(z + hop, NZ)

    def ring_copy(n, direction, hop):
        half = direction if hop == NZ // 2 else None
        ref = piece(n, source_of(direction, hop - 1), c, half)
        return pltpu.make_async_remote_copy(
            src_ref=ref, dst_ref=ref,
            send_sem=ring_send.at[n, direction, hop - 1],
            recv_sem=ring_recv.at[n, direction, hop - 1],
            device_id=(ex, ey, up if direction == 0 else down, c), device_id_type=MESH)

    def ring_arrival(n, direction, hop):
        half = direction if hop == NZ // 2 else None
        ref = piece(n, source_of(direction, hop), c, half)
        return pltpu.make_async_remote_copy(
            src_ref=ref, dst_ref=ref,
            send_sem=ring_send.at[n, direction, hop - 1],
            recv_sem=ring_recv.at[n, direction, hop - 1],
            device_id=(ex, ey, up if direction == 0 else down, c), device_id_type=MESH)

    def pair_slots():
        slots = [(0, 0)]
        for hop in range(1, NZ // 2):
            slots += [(0, hop), (1, hop)]
        return slots + [(0, NZ // 2)]

    slot_of = {s: k for k, s in enumerate(pair_slots())}

    def pair_copy(n, direction, hop, core):
        ref = piece(n, source_of(direction, hop), core)
        k = slot_of[(direction, hop)]
        return pltpu.make_async_remote_copy(
            src_ref=ref, dst_ref=ref,
            send_sem=pair_send.at[n, k], recv_sem=pair_recv.at[n, k],
            device_id=(ex, ey, z, other), device_id_type=MESH)

    barrier = pltpu.get_barrier_semaphore()

    x_sides = [(lax.rem(ex + d, NX), ey, z, c) for d in (1, NX - 1)]
    y_sides = [(ex, lax.rem(ey + d, NY), z, c) for d in (1, NY - 1)]
    z_sides = [(ex, ey, up, c), (ex, ey, down, c), (ex, ey, z, other)]

    def signal_all(sem, devices):
        for device in devices:
            pl.semaphore_signal(sem, inc=1, device_id=device, device_id_type=MESH)

    signal_all(barrier, z_sides + x_sides + y_sides)
    def cross_copy(n, direction, core, hop):
        ref = piece(n, source_of(direction, hop), core, direction)
        return pltpu.make_async_remote_copy(
            src_ref=ref, dst_ref=ref,
            send_sem=cross_send.at[direction], recv_sem=cross_recv.at[direction],
            device_id=(ex, ey, up if direction == 0 else down, other), device_id_type=MESH)

    local_copy(0).start()
    inputs = [(tokens_ref, tok_buf), (routes_hbm, routes_ref), (modality_hbm, modality_ref),
              (router_hbm, router_ref)]
    input_copies = [
        pltpu.make_async_copy(source, target, tok_sem.at[k])
        for k, (source, target) in enumerate(inputs)]
    for n in range(1, chunks):
        local_copy(n).start()
        if n == 1:
            for copy in input_copies:
                copy.start()
    pl.semaphore_wait(barrier, len(z_sides + x_sides + y_sides))

    def send_own(n):
        local_copy(n).wait()
        for direction in range(2):
            ring_copy(n, direction, 1).start()
        pair_copy(n, 0, 0, c).start()

    send_own(0)
    send_own(1)
    signal_all(row_in.at[0], x_sides)

    for copy in input_copies:
        copy.wait()
    tok = tok_buf[...]
    logits = lax.dot_general(
        router_ref[...], tok, (((1,), (1,)), ((), ())), preferred_element_type=jnp.float32)
    micro = toks // 2
    route = jnp.concatenate([routes_ref[0], routes_ref[1]], axis=1)
    modality = jnp.concatenate([modality_ref[0:1, :], modality_ref[1:2, :]], axis=1)
    expert_id = lax.broadcasted_iota(jnp.int32, (experts, toks), 0)
    onehot = (route == expert_id).astype(jnp.float32)
    chosen = jnp.sum(logits * onehot, axis=0, keepdims=True)
    gating = 1.0 / (1.0 + jnp.exp(-chosen))
    for m in range(2):
        spread = jnp.broadcast_to(gating[:, m * micro:(m + 1) * micro], (micro, micro))
        gate[m * micro:(m + 1) * micro, :] = spread.T
    row_i = lax.broadcasted_iota(jnp.int32, (toks, toks), 0)
    col_i = lax.broadcasted_iota(jnp.int32, (toks, toks), 1)
    first = jnp.where(col_i >= micro, micro, 0)
    earlier = ((row_i <= col_i) & (row_i >= first)).astype(jnp.bfloat16)
    running = jnp.dot(onehot.astype(jnp.bfloat16), earlier, preferred_element_type=jnp.float32)
    spot = jnp.sum(
        (running - 1.0 + expert_id.astype(jnp.float32) * block) * onehot, axis=0, keepdims=True)
    token_id = lax.broadcasted_iota(jnp.int32, (1, toks), 1)
    spot = spot + jnp.where(token_id >= micro, block // 2, 0).astype(jnp.float32)
    slots = lax.broadcasted_iota(jnp.int32, (experts * block, toks), 0).astype(jnp.float32)
    place = (spot == slots).astype(jnp.bfloat16)
    placer[...] = place.T
    buffer[...] = jnp.dot(place, tok, preferred_element_type=jnp.float32).astype(jnp.bfloat16)

    exps = jnp.exp(logits)
    probs = exps / jnp.sum(exps, axis=0, keepdims=True)
    stat[...] = jnp.zeros(stat.shape, jnp.float32)
    for k in range(2):
        modal = (modality == k).astype(jnp.float32)
        stat[:, k:k + 1] = jnp.sum(onehot * modal, axis=1, keepdims=True)
        stat[:, 2 + k:3 + k] = jnp.sum(probs * modal, axis=1, keepdims=True)
        stat[:, 4 + k:5 + k] = jnp.sum(
            jnp.broadcast_to(modal, (experts, toks)), axis=1, keepdims=True)

    pl.semaphore_wait(row_in.at[0], 2)
    signal_all(row_in.at[1], y_sides)
    pl.semaphore_wait(row_in.at[1], 2)
    signal_all(row_in.at[2], y_sides)

    def dispatch(j, carry):
        p, device = plane_peer(j)
        pltpu.make_async_remote_copy(
            src_ref=buffer.at[pl.ds(pl.multiple_of(p * block, 16), block)],
            dst_ref=rows.at[pl.ds(pl.multiple_of(me * block, 16), block)],
            send_sem=disp_send, recv_sem=disp_recv,
            device_id=device, device_id_type=MESH).start()
        return carry

    own_rows = pl.ds(pl.multiple_of(me * block, 16), block)
    rows[own_rows, :] = buffer[own_rows, :]
    pl.semaphore_wait(row_in.at[2], 2)
    lax.fori_loop(1, experts, dispatch, 0)

    def stat_plane(j, carry):
        _, device = plane_peer(j)
        pltpu.make_async_remote_copy(
            src_ref=stat, dst_ref=stat_rx.at[me], send_sem=stat_send.at[0],
            recv_sem=stat_recv.at[0], device_id=device, device_id_type=MESH).start()
        return carry

    def stat_dp(j, carry):
        _, device = dp_peer(j)
        pltpu.make_async_remote_copy(
            src_ref=stat_sum, dst_ref=stat_rx2.at[mine], send_sem=stat_send.at[1],
            recv_sem=stat_recv.at[1], device_id=device, device_id_type=MESH).start()
        return carry

    stat_rx[me] = stat[...]
    lax.fori_loop(1, experts, stat_plane, 0)

    def take(ref, sem):
        pltpu.make_async_copy(ref, ref, sem).wait()

    others = (experts - 1) * block

    def first_product(n):
        tile = 256

        def body(t, carry):
            at = pl.ds(pl.multiple_of(t * tile, tile), tile)
            acc = jnp.dot(rows[...], win[n, :, at], preferred_element_type=jnp.float32)
            to = pl.ds(pl.multiple_of(n * cols_in + t * tile, tile), tile)
            hidden[:, to] = gelu(acc).astype(jnp.bfloat16)
            return carry

        lax.fori_loop(0, cols_in // tile, body, 0)

    def apart(d):
        return min(d[0], NX - d[0]) + min(d[1], NY - d[1])

    steps = [(dx, dy) for dx in range(NX) for dy in range(NY) if (dx, dy) != (0, 0)]
    steps.sort(key=apart, reverse=True)

    def send_back(n):
        for dx, dy in steps:
            px, py = lax.rem(ex + dx, NX), lax.rem(ey + dy, NY)
            p, device = px * NY + py, (px, py, z, c)
            pltpu.make_async_remote_copy(
                src_ref=served[n].at[pl.ds(pl.multiple_of(p * block, 16), block)],
                dst_ref=returned[n].at[pl.ds(pl.multiple_of(me * block, 16), block)],
                send_sem=back_send.at[n], recv_sem=back_recv.at[n],
                device_id=device, device_id_type=MESH).start()

    def combine(n):
        take(returned[n].at[pl.ds(0, others)], back_recv.at[n])
        combined = jnp.dot(
            placer[...], returned[n][...], preferred_element_type=jnp.float32)
        mixed_ref[:, columns(n)] = (combined * gate[:, 0:1]).astype(jnp.bfloat16)

    far_side = lax.rem(z + NZ // 2, NZ) // (NZ // 2)
    half_ff = hidden.shape[1] // 2

    def half_product(n, side):
        at = pl.ds(pl.multiple_of(side * half_ff, 128), half_ff)
        return jnp.dot(hidden[:, at], wout[n][at, :], preferred_element_type=jnp.float32)

    def second_product_start(n):
        partial[:, pl.ds(0, WIDTHS_OUT[n])] = half_product(n, 1 - far_side)

    def second_product(n):
        acc = partial[:, pl.ds(0, WIDTHS_OUT[n])] + half_product(n, far_side)
        served[n][...] = acc.astype(jnp.bfloat16)
        returned[n][own_rows, :] = served[n][own_rows, :]
        send_back(n)
        if n > 1:
            combine(n - 2)

    def product(n):
        if n < chunks - 1:
            pair_copy(n, 0, last, other).wait_recv()
        if n == chunks - 1:
            for direction in range(2):
                cross_copy(n, direction, other, last).wait_recv()
        if n < CHUNKS_IN:
            first_product(n)
        else:
            second_product(n - CHUNKS_IN)

    last = NZ // 2
    for r in range(1, chunks + last):
        if r < chunks - 1:
            send_own(r + 1)
        for hop in range(1, last):
            n = r - hop
            if not 0 <= n < chunks:
                continue
            for direction in range(2):
                ring_arrival(n, direction, hop).wait_recv()
                ring_copy(n, direction, hop + 1).start()
                if n == chunks - 1 and hop == last - 1:
                    cross_copy(n, direction, c, hop).start()
                pair_copy(n, direction, hop, c).start()
        n = r - last
        if n >= 0:
            for (direction, hop) in pair_slots()[:-1]:
                pair_copy(n, direction, hop, other).wait_recv()
            if n >= CHUNKS_IN:
                second_product_start(n - CHUNKS_IN)
            for direction in range(2):
                ring_arrival(n, direction, last).wait_recv()
            if n < chunks - 1:
                pair_copy(n, 0, last, c).start()
        if n == 0:
            take(rows.at[pl.ds(0, others)], disp_recv)
            take(stat_rx.at[pl.ds(0, experts - 1)], stat_recv.at[0])
            total = stat_rx[0]
            for p in range(1, experts):
                total = total + stat_rx[p]
            stat_sum[...] = total
            stat_rx2[mine] = total
        if n >= 0:
            product(n)
        if n == 1:
            lax.fori_loop(1, dps, stat_dp, 0)
        if n == 3:
            take(stat_rx2.at[pl.ds(0, dps - 1)], stat_recv.at[1])
            total = stat_rx2[0]
            for p in range(1, dps):
                total = total + stat_rx2[p]
            flat = total.T
            modal_counts = flat[4:6, 0:experts]
            load_ref[0] = experts * flat[0:2, 0:experts] / modal_counts
            load_ref[1] = experts * flat[2:4, 0:experts] / modal_counts

    for n in range(chunks):
        for direction in range(2):
            for hop in range(1, last + 1):
                ring_copy(n, direction, hop).wait_send()
        for (direction, hop) in pair_slots():
            if n < chunks - 1 or hop < last:
                pair_copy(n, direction, hop, c).wait_send()
    for direction in range(2):
        cross_copy(chunks - 1, direction, c, last - 1).wait_send()
    take(buffer.at[pl.ds(0, others)], disp_send)
    take(stat_rx.at[pl.ds(0, experts - 1)], stat_send.at[0])
    take(stat_rx2.at[pl.ds(0, dps - 1)], stat_send.at[1])
    combine(CHUNKS_OUT - 2)
    combine(CHUNKS_OUT - 1)
    for n in range(CHUNKS_OUT):
        take(served[n].at[pl.ds(0, others)], back_send.at[n])


def on_device(tokens, modality, routes, router, w_in, w_out):
    micro_count, tok_count, model_width = tokens.shape
    experts = router.shape[1]
    capacity = 2 * tok_count // experts
    toks = micro_count * tok_count
    block = micro_count * capacity
    slots = experts * block
    ff = w_in.shape[2]
    cols_in = ff // CHUNKS_IN
    chunks = CHUNKS_IN + CHUNKS_OUT
    half = NZ // 2
    bf16, f32 = jnp.bfloat16, jnp.float32
    vmem = pl.BlockSpec(memory_space=pltpu.VMEM)
    hbm = pl.BlockSpec(memory_space=pltpu.HBM)
    dma = pltpu.SemaphoreType.DMA
    mixed, load = pl.pallas_call(
        layer_kernel,
        out_shape=(
            pltpu.VMEM((toks, model_width), bf16),
            pltpu.VMEM((2, 2, experts), f32),
        ),
        in_specs=[hbm] * 6,
        out_specs=(vmem, vmem),
        scratch_shapes=[
            pltpu.VMEM((micro_count, 1, tok_count), jnp.int32),
            pltpu.VMEM((micro_count, tok_count), jnp.int32),
            pltpu.VMEM((experts, model_width), bf16),
            pltpu.VMEM((CHUNKS_IN, model_width, cols_in), bf16),
            [pltpu.VMEM((ff, w), bf16) for w in WIDTHS_OUT],
            pltpu.VMEM((toks, model_width), bf16),
            pltpu.VMEM((toks, slots), bf16),
            pltpu.VMEM((toks, 128), f32),
            pltpu.VMEM((slots, model_width), bf16),
            pltpu.VMEM((slots, model_width), bf16),
            pltpu.VMEM((slots, ff), bf16),
            pltpu.VMEM((slots, max(WIDTHS_OUT)), f32),
            [pltpu.VMEM((slots, w), bf16) for w in WIDTHS_OUT],
            [pltpu.VMEM((slots, w), bf16) for w in WIDTHS_OUT],
            pltpu.VMEM((experts, 128), f32),
            pltpu.VMEM((experts, experts, 128), f32),
            pltpu.VMEM((experts, 128), f32),
            pltpu.VMEM((NZ * NC, experts, 128), f32),
            dma((4,)),
            dma((chunks,)),
            dma((chunks, 2, half)),
            dma((chunks, 2, half)),
            dma((chunks, NZ)),
            dma((chunks, NZ)),
            dma,
            dma,
            dma((CHUNKS_OUT,)),
            dma((CHUNKS_OUT,)),
            dma((2,)),
            dma((2,)),
            pltpu.SemaphoreType.REGULAR((3,)),
            dma((2,)),
            dma((2,)),
        ],
        compiler_params=pltpu.CompilerParams(
            collective_id=0, has_side_effects=True, vmem_limit_bytes=VMEM_BYTES
        ),
        name="layer",
    )(
        tokens.reshape(toks, model_width),
        jnp.transpose(routes, (0, 2, 1)),
        modality,
        router.T,
        w_in,
        w_out,
    )
    return mixed.reshape(tokens.shape), load


def solution(mesh):
    torus = Mesh(mesh.devices.reshape(NX, NY, NZ, NC), AXES)
    expert, dp, both = AXES[:2], AXES[2:], AXES
    in_specs = (
        P(None, both, None), P(None, both), P(None, both, None), P(),
        P(expert, dp, None), P(expert, dp, None),
    )
    out_specs = (P(None, both, None), P())
    return jax.shard_map(
        on_device, mesh=torus, in_specs=in_specs, out_specs=out_specs, check_vma=False
    )
```

```python
import functools
import math

import jax
import jax.numpy as jnp
from jax import lax
from jax.experimental import pallas as pl
from jax.experimental.pallas import tpu as pltpu
from jax.sharding import Mesh
from jax.sharding import PartitionSpec as P

NX, NY, NZ, NC = 4, 4, 8, 2
AXES = ("expert_0", "expert_1", "dp_0", "dp_1")
MESH = pl.DeviceIdType.MESH
CHUNKS_IN = 2
WIDTHS_OUT = (512, 384, 256, 128)
CHUNKS_OUT = len(WIDTHS_OUT)
VMEM_BYTES = 65900000
GELU_C = math.sqrt(2.0 / math.pi)


def gelu(v):
    return 0.5 * v * (1.0 + jnp.tanh(GELU_C * (v + 0.044715 * (v * v * v))))


def layer_kernel(
    tokens_ref, routes_hbm, modality_hbm, router_hbm, w_in_ref, w_out_ref,
    mixed_ref, load_ref,
    routes_ref, modality_ref, router_ref, win, wout, tok_buf, placer, gate, buffer, rows, hidden, partial, served, returned,
    stat, stat_rx, stat_sum, stat_rx2,
    tok_sem, local_sem, ring_send, ring_recv, pair_send, pair_recv,
    disp_send, disp_recv, back_send, back_recv, stat_send, stat_recv, row_in, cross_send, cross_recv,
):
    shard_in = w_in_ref.shape[1]
    shard_out = w_out_ref.shape[1]
    width = tokens_ref.shape[1]
    toks = tokens_ref.shape[0]
    experts = router_hbm.shape[0]
    block = rows.shape[0] // experts
    cols_in = win.shape[2]
    chunks = CHUNKS_IN + CHUNKS_OUT
    dps = NZ * NC

    ex, ey = lax.axis_index("expert_0"), lax.axis_index("expert_1")
    z, c = lax.axis_index("dp_0"), lax.axis_index("dp_1")
    me = ex * NY + ey
    mine = z * NC + c
    up, down = lax.rem(z + 1, NZ), lax.rem(z + NZ - 1, NZ)
    other = 1 - c

    def plane_peer(j):
        p = lax.rem(me + j, experts)
        return p, (p // NY, lax.rem(p, NY), z, c)

    def dp_peer(j):
        p = lax.rem(mine + j, dps)
        return p, (ex, ey, p // NC, lax.rem(p, NC))

    def piece(n, source_z, core, half=None):
        shard = source_z * NC + core
        if n < CHUNKS_IN:
            view = win.at[n, pl.ds(pl.multiple_of(shard * shard_in, 16), shard_in)]
            if half is not None:
                view = win.at[
                    n, pl.ds(pl.multiple_of(shard * shard_in, 16), shard_in),
                    pl.ds(half * (cols_in // 2), cols_in // 2)]
            return view
        if half is None:
            return wout[n - CHUNKS_IN].at[pl.ds(pl.multiple_of(shard * shard_out, 16), shard_out)]
        rows_half = shard_out // 2
        return wout[n - CHUNKS_IN].at[
            pl.ds(pl.multiple_of(shard * shard_out + half * rows_half, 16), rows_half)]

    def columns(n):
        return pl.ds(sum(WIDTHS_OUT[:n]), WIDTHS_OUT[n])

    def local_copy(n):
        if n < CHUNKS_IN:
            source = w_in_ref.at[0, :, pl.ds(n * cols_in, cols_in)]
        else:
            source = w_out_ref.at[0, :, columns(n - CHUNKS_IN)]
        return pltpu.make_async_copy(source, piece(n, z, c), local_sem.at[n])

    def source_of(direction, hop):
        return lax.rem(z + NZ - hop, NZ) if direction == 0 else lax.rem(z + hop, NZ)

    def ring_copy(n, direction, hop):
        half = direction if hop == NZ // 2 else None
        ref = piece(n, source_of(direction, hop - 1), c, half)
        return pltpu.make_async_remote_copy(
            src_ref=ref, dst_ref=ref,
            send_sem=ring_send.at[n, direction, hop - 1],
            recv_sem=ring_recv.at[n, direction, hop - 1],
            device_id=(ex, ey, up if direction == 0 else down, c), device_id_type=MESH)

    def ring_arrival(n, direction, hop):
        half = direction if hop == NZ // 2 else None
        ref = piece(n, source_of(direction, hop), c, half)
        return pltpu.make_async_remote_copy(
            src_ref=ref, dst_ref=ref,
            send_sem=ring_send.at[n, direction, hop - 1],
            recv_sem=ring_recv.at[n, direction, hop - 1],
            device_id=(ex, ey, up if direction == 0 else down, c), device_id_type=MESH)

    def pair_slots():
        slots = [(0, 0)]
        for hop in range(1, NZ // 2):
            slots += [(0, hop), (1, hop)]
        return slots + [(0, NZ // 2)]

    slot_of = {s: k for k, s in enumerate(pair_slots())}

    def pair_copy(n, direction, hop, core):
        ref = piece(n, source_of(direction, hop), core)
        k = slot_of[(direction, hop)]
        return pltpu.make_async_remote_copy(
            src_ref=ref, dst_ref=ref,
            send_sem=pair_send.at[n, k], recv_sem=pair_recv.at[n, k],
            device_id=(ex, ey, z, other), device_id_type=MESH)

    barrier = pltpu.get_barrier_semaphore()

    x_sides = [(lax.rem(ex + d, NX), ey, z, c) for d in (1, NX - 1)]
    y_sides = [(ex, lax.rem(ey + d, NY), z, c) for d in (1, NY - 1)]
    z_sides = [(ex, ey, up, c), (ex, ey, down, c), (ex, ey, z, other)]

    def signal_all(sem, devices):
        for device in devices:
            pl.semaphore_signal(sem, inc=1, device_id=device, device_id_type=MESH)

    signal_all(barrier, z_sides + x_sides + y_sides)
    def cross_copy(n, direction, core, hop):
        ref = piece(n, source_of(direction, hop), core, direction)
        return pltpu.make_async_remote_copy(
            src_ref=ref, dst_ref=ref,
            send_sem=cross_send.at[direction], recv_sem=cross_recv.at[direction],
            device_id=(ex, ey, up if direction == 0 else down, other), device_id_type=MESH)

    local_copy(0).start()
    inputs = [(tokens_ref, tok_buf), (routes_hbm, routes_ref), (modality_hbm, modality_ref),
              (router_hbm, router_ref)]
    input_copies = [
        pltpu.make_async_copy(source, target, tok_sem.at[k])
        for k, (source, target) in enumerate(inputs)]
    for n in range(1, chunks):
        local_copy(n).start()
        if n == 1:
            for copy in input_copies:
                copy.start()
    pl.semaphore_wait(barrier, len(z_sides + x_sides + y_sides))

    def send_own(n):
        local_copy(n).wait()
        for direction in range(2):
            ring_copy(n, direction, 1).start()
        pair_copy(n, 0, 0, c).start()

    send_own(0)
    send_own(1)
    signal_all(row_in.at[0], x_sides)

    for copy in input_copies:
        copy.wait()
    tok = tok_buf[...]
    logits = lax.dot_general(
        router_ref[...], tok, (((1,), (1,)), ((), ())), preferred_element_type=jnp.float32)
    micro = toks // 2
    route = jnp.concatenate([routes_ref[0], routes_ref[1]], axis=1)
    modality = jnp.concatenate([modality_ref[0:1, :], modality_ref[1:2, :]], axis=1)
    expert_id = lax.broadcasted_iota(jnp.int32, (experts, toks), 0)
    onehot = (route == expert_id).astype(jnp.float32)
    chosen = jnp.sum(logits * onehot, axis=0, keepdims=True)
    gating = 1.0 / (1.0 + jnp.exp(-chosen))
    for m in range(2):
        spread = jnp.broadcast_to(gating[:, m * micro:(m + 1) * micro], (micro, micro))
        gate[m * micro:(m + 1) * micro, :] = spread.T
    row_i = lax.broadcasted_iota(jnp.int32, (toks, toks), 0)
    col_i = lax.broadcasted_iota(jnp.int32, (toks, toks), 1)
    first = jnp.where(col_i >= micro, micro, 0)
    earlier = ((row_i <= col_i) & (row_i >= first)).astype(jnp.bfloat16)
    running = jnp.dot(onehot.astype(jnp.bfloat16), earlier, preferred_element_type=jnp.float32)
    spot = jnp.sum(
        (running - 1.0 + expert_id.astype(jnp.float32) * block) * onehot, axis=0, keepdims=True)
    token_id = lax.broadcasted_iota(jnp.int32, (1, toks), 1)
    spot = spot + jnp.where(token_id >= micro, block // 2, 0).astype(jnp.float32)
    slots = lax.broadcasted_iota(jnp.int32, (experts * block, toks), 0).astype(jnp.float32)
    place = (spot == slots).astype(jnp.bfloat16)
    placer[...] = place.T
    buffer[...] = jnp.dot(place, tok, preferred_element_type=jnp.float32).astype(jnp.bfloat16)

    exps = jnp.exp(logits)
    probs = exps / jnp.sum(exps, axis=0, keepdims=True)
    stat[...] = jnp.zeros(stat.shape, jnp.float32)
    for k in range(2):
        modal = (modality == k).astype(jnp.float32)
        stat[:, k:k + 1] = jnp.sum(onehot * modal, axis=1, keepdims=True)
        stat[:, 2 + k:3 + k] = jnp.sum(probs * modal, axis=1, keepdims=True)
        stat[:, 4 + k:5 + k] = jnp.sum(
            jnp.broadcast_to(modal, (experts, toks)), axis=1, keepdims=True)

    pl.semaphore_wait(row_in.at[0], 2)
    signal_all(row_in.at[1], y_sides)
    pl.semaphore_wait(row_in.at[1], 2)
    signal_all(row_in.at[2], y_sides)

    def dispatch(j, carry):
        p, device = plane_peer(j)
        pltpu.make_async_remote_copy(
            src_ref=buffer.at[pl.ds(pl.multiple_of(p * block, 16), block)],
            dst_ref=rows.at[pl.ds(pl.multiple_of(me * block, 16), block)],
            send_sem=disp_send, recv_sem=disp_recv,
            device_id=device, device_id_type=MESH).start()
        return carry

    own_rows = pl.ds(pl.multiple_of(me * block, 16), block)
    rows[own_rows, :] = buffer[own_rows, :]
    pl.semaphore_wait(row_in.at[2], 2)
    lax.fori_loop(1, experts, dispatch, 0)

    def stat_plane(j, carry):
        _, device = plane_peer(j)
        pltpu.make_async_remote_copy(
            src_ref=stat, dst_ref=stat_rx.at[me], send_sem=stat_send.at[0],
            recv_sem=stat_recv.at[0], device_id=device, device_id_type=MESH).start()
        return carry

    def stat_dp(j, carry):
        _, device = dp_peer(j)
        pltpu.make_async_remote_copy(
            src_ref=stat_sum, dst_ref=stat_rx2.at[mine], send_sem=stat_send.at[1],
            recv_sem=stat_recv.at[1], device_id=device, device_id_type=MESH).start()
        return carry

    stat_rx[me] = stat[...]
    lax.fori_loop(1, experts, stat_plane, 0)

    def take(ref, sem):
        pltpu.make_async_copy(ref, ref, sem).wait()

    others = (experts - 1) * block

    def first_product(n):
        tile = 256

        def body(t, carry):
            at = pl.ds(pl.multiple_of(t * tile, tile), tile)
            acc = jnp.dot(rows[...], win[n, :, at], preferred_element_type=jnp.float32)
            to = pl.ds(pl.multiple_of(n * cols_in + t * tile, tile), tile)
            hidden[:, to] = gelu(acc).astype(jnp.bfloat16)
            return carry

        lax.fori_loop(0, cols_in // tile, body, 0)

    def apart(d):
        return min(d[0], NX - d[0]) + min(d[1], NY - d[1])

    steps = [(dx, dy) for dx in range(NX) for dy in range(NY) if (dx, dy) != (0, 0)]
    steps.sort(key=apart, reverse=True)

    def send_back(n):
        for dx, dy in steps:
            px, py = lax.rem(ex + dx, NX), lax.rem(ey + dy, NY)
            p, device = px * NY + py, (px, py, z, c)
            pltpu.make_async_remote_copy(
                src_ref=served[n].at[pl.ds(pl.multiple_of(p * block, 16), block)],
                dst_ref=returned[n].at[pl.ds(pl.multiple_of(me * block, 16), block)],
                send_sem=back_send.at[n], recv_sem=back_recv.at[n],
                device_id=device, device_id_type=MESH).start()

    def combine(n):
        take(returned[n].at[pl.ds(0, others)], back_recv.at[n])
        combined = jnp.dot(
            placer[...], returned[n][...], preferred_element_type=jnp.float32)
        mixed_ref[:, columns(n)] = (combined * gate[:, 0:1]).astype(jnp.bfloat16)

    far_side = lax.rem(z + NZ // 2, NZ) // (NZ // 2)
    half_ff = hidden.shape[1] // 2

    def half_product(n, side):
        at = pl.ds(pl.multiple_of(side * half_ff, 128), half_ff)
        return jnp.dot(hidden[:, at], wout[n][at, :], preferred_element_type=jnp.float32)

    def second_product_start(n):
        partial[:, pl.ds(0, WIDTHS_OUT[n])] = half_product(n, 1 - far_side)

    def second_product(n):
        acc = partial[:, pl.ds(0, WIDTHS_OUT[n])] + half_product(n, far_side)
        served[n][...] = acc.astype(jnp.bfloat16)
        returned[n][own_rows, :] = served[n][own_rows, :]
        send_back(n)
        if n > 1:
            combine(n - 2)

    def product(n):
        if n < chunks - 1:
            pair_copy(n, 0, last, other).wait_recv()
        if n == chunks - 1:
            for direction in range(2):
                cross_copy(n, direction, other, last).wait_recv()
        if n < CHUNKS_IN:
            first_product(n)
        else:
            second_product(n - CHUNKS_IN)

    last = NZ // 2
    for r in range(1, chunks + last):
        if r < chunks - 1:
            send_own(r + 1)
        for hop in range(1, last):
            n = r - hop
            if not 0 <= n < chunks:
                continue
            for direction in range(2):
                ring_arrival(n, direction, hop).wait_recv()
                ring_copy(n, direction, hop + 1).start()
                if n == chunks - 1 and hop == last - 1:
                    cross_copy(n, direction, c, hop).start()
                pair_copy(n, direction, hop, c).start()
        n = r - last
        if n >= 0:
            for (direction, hop) in pair_slots()[:-1]:
                pair_copy(n, direction, hop, other).wait_recv()
            if n >= CHUNKS_IN:
                second_product_start(n - CHUNKS_IN)
            for direction in range(2):
                ring_arrival(n, direction, last).wait_recv()
            if n < chunks - 1:
                pair_copy(n, 0, last, c).start()
        if n == 0:
            take(rows.at[pl.ds(0, others)], disp_recv)
            take(stat_rx.at[pl.ds(0, experts - 1)], stat_recv.at[0])
            total = stat_rx[0]
            for p in range(1, experts):
                total = total + stat_rx[p]
            stat_sum[...] = total
            stat_rx2[mine] = total
        if n >= 0:
            product(n)
        if n == 1:
            lax.fori_loop(1, dps, stat_dp, 0)
        if n == 3:
            take(stat_rx2.at[pl.ds(0, dps - 1)], stat_recv.at[1])
            total = stat_rx2[0]
            for p in range(1, dps):
                total = total + stat_rx2[p]
            flat = total.T
            modal_counts = flat[4:6, 0:experts]
            load_ref[0] = experts * flat[0:2, 0:experts] / modal_counts
            load_ref[1] = experts * flat[2:4, 0:experts] / modal_counts

    for n in range(chunks):
        for direction in range(2):
            for hop in range(1, last + 1):
                ring_copy(n, direction, hop).wait_send()
        for (direction, hop) in pair_slots():
            if n < chunks - 1 or hop < last:
                pair_copy(n, direction, hop, c).wait_send()
    for direction in range(2):
        cross_copy(chunks - 1, direction, c, last - 1).wait_send()
    take(buffer.at[pl.ds(0, others)], disp_send)
    take(stat_rx.at[pl.ds(0, experts - 1)], stat_send.at[0])
    take(stat_rx2.at[pl.ds(0, dps - 1)], stat_send.at[1])
    combine(CHUNKS_OUT - 2)
    combine(CHUNKS_OUT - 1)
    for n in range(CHUNKS_OUT):
        take(served[n].at[pl.ds(0, others)], back_send.at[n])


def hand_over(mixed_ref, load_ref, mixed_out, load_out, sem):
    copies = [
        pltpu.make_async_copy(mixed_ref, mixed_out, sem.at[0]),
        pltpu.make_async_copy(load_ref, load_out, sem.at[1]),
    ]
    for copy in copies:
        copy.start()
    for copy in copies:
        copy.wait()


def on_device(tokens, modality, routes, router, w_in, w_out):
    micro_count, tok_count, model_width = tokens.shape
    experts = router.shape[1]
    capacity = 2 * tok_count // experts
    toks = micro_count * tok_count
    block = micro_count * capacity
    slots = experts * block
    ff = w_in.shape[2]
    cols_in = ff // CHUNKS_IN
    chunks = CHUNKS_IN + CHUNKS_OUT
    half = NZ // 2
    bf16, f32 = jnp.bfloat16, jnp.float32
    vmem = pl.BlockSpec(memory_space=pltpu.VMEM)
    hbm = pl.BlockSpec(memory_space=pltpu.HBM)
    dma = pltpu.SemaphoreType.DMA
    mixed, load = pl.pallas_call(
        layer_kernel,
        out_shape=(
            pltpu.VMEM((toks, model_width), bf16),
            pltpu.VMEM((2, 2, experts), f32),
        ),
        in_specs=[hbm] * 6,
        out_specs=(vmem, vmem),
        scratch_shapes=[
            pltpu.VMEM((micro_count, 1, tok_count), jnp.int32),
            pltpu.VMEM((micro_count, tok_count), jnp.int32),
            pltpu.VMEM((experts, model_width), bf16),
            pltpu.VMEM((CHUNKS_IN, model_width, cols_in), bf16),
            [pltpu.VMEM((ff, w), bf16) for w in WIDTHS_OUT],
            pltpu.VMEM((toks, model_width), bf16),
            pltpu.VMEM((toks, slots), bf16),
            pltpu.VMEM((toks, 128), f32),
            pltpu.VMEM((slots, model_width), bf16),
            pltpu.VMEM((slots, model_width), bf16),
            pltpu.VMEM((slots, ff), bf16),
            pltpu.VMEM((slots, max(WIDTHS_OUT)), f32),
            [pltpu.VMEM((slots, w), bf16) for w in WIDTHS_OUT],
            [pltpu.VMEM((slots, w), bf16) for w in WIDTHS_OUT],
            pltpu.VMEM((experts, 128), f32),
            pltpu.VMEM((experts, experts, 128), f32),
            pltpu.VMEM((experts, 128), f32),
            pltpu.VMEM((NZ * NC, experts, 128), f32),
            dma((4,)),
            dma((chunks,)),
            dma((chunks, 2, half)),
            dma((chunks, 2, half)),
            dma((chunks, NZ)),
            dma((chunks, NZ)),
            dma,
            dma,
            dma((CHUNKS_OUT,)),
            dma((CHUNKS_OUT,)),
            dma((2,)),
            dma((2,)),
            pltpu.SemaphoreType.REGULAR((3,)),
            dma((2,)),
            dma((2,)),
        ],
        compiler_params=pltpu.CompilerParams(
            collective_id=0, has_side_effects=True, vmem_limit_bytes=VMEM_BYTES
        ),
        name="layer",
    )(
        tokens.reshape(toks, model_width),
        jnp.transpose(routes, (0, 2, 1)),
        modality,
        router.T,
        w_in,
        w_out,
    )
    mixed, load = pl.pallas_call(
        hand_over,
        out_shape=(
            jax.ShapeDtypeStruct((toks, model_width), bf16),
            jax.ShapeDtypeStruct((2, 2, experts), f32),
        ),
        in_specs=[vmem, vmem],
        out_specs=(hbm, hbm),
        scratch_shapes=[dma((2,))],
        compiler_params=pltpu.CompilerParams(vmem_limit_bytes=4 * 1024 * 1024),
        name="hand_over",
    )(mixed, load)
    return mixed.reshape(tokens.shape), load


def solution(mesh):
    torus = Mesh(mesh.devices.reshape(NX, NY, NZ, NC), AXES)
    expert, dp, both = AXES[:2], AXES[2:], AXES
    in_specs = (
        P(None, both, None), P(None, both), P(None, both, None), P(),
        P(expert, dp, None), P(expert, dp, None),
    )
    out_specs = (P(None, both, None), P())
    return jax.shard_map(
        on_device, mesh=torus, in_specs=in_specs, out_specs=out_specs, check_vma=False
    )
```
